256 devices in a mesh: gx: 128 (over x, y_lo, z, core), gy: 2 (over y_hi).
Axes of the slice: x: 4, y: 4 (y_hi: 2, y_lo: 2; y = y_hi * 2 + y_lo), z: 8, core: 2. Of those that a mesh axis runs over, the one named last changes fastest.
Arguments:
- particles: float32 [64, 2, 512, 1024], P(None, None, 'gx', 'gy'), may hold values from -32 to 32, as said below
- background: float32 [2, 512, 1024], P(None, 'gx', 'gy'), may hold values from -6 to 6
- obs_tile: int32 [128, 256], P('gx', 'gy'), may hold values from 0 to 127
- obs_mask: int32 [16, 128, 256], P(None, 'gx', 'gy'), may hold values 0 or 1
- obs_value: float32 [128, 256], P('gx', 'gy'), may hold values from -6 to 6
- obs_var: float32 [128, 256], P('gx', 'gy'), may hold values from 0.1 to 1
Outputs:
- analysis: float32 [64, 2, 512, 1024], P(None, None, 'gx', 'gy')
The draws below stay inside these ranges and needn't reach their ends.
Inputs may be any that keep to these rules, and one draw needn't show every extreme that they name: `particles`: each particle is a field of order one to a few. `obs_tile`: an observation's value names tile row t // 128 and tile column t % (128) of its slab.
All inputs are finite; a program needn't handle non-finite values. No bound on the sum of `obs_mask` on one device may be relied on, other than what follows from the above.
Results may differ from the reference program's by a relative error of at most 0.0001.
Values sent between devices are 32-bit elements; how exact they have to be, the bound alone decides.
No kernel may reach another device: no remote copies, remote signals or barrier semaphores. Data moves between devices by JAX's collectives and lax.ppermute only.
A program may use at most 64 MiB of HBM per device.

```python
import math
import jax
import jax.numpy as jnp
from jax import lax

NP = 64
LAYERS = 2
STEPS = 2
TILE = 4
CX = 4
CY = 512
OBS_DEV = 128
NX = 512
NY = 1024
TILES_DEV = 128
N_GX = 128
N_GY = 2


def draw_particles(key, part):
    keys = jax.random.split(jax.random.fold_in(key, 11), 3)
    shape = (NP, LAYERS, NX, NY)
    spread = jnp.exp(jax.random.uniform(keys[0], (NP, 1, 1, 1), jnp.float32, math.log(0.5), math.log(2.0)))
    rough = jnp.exp(jax.random.uniform(keys[1], shape, jnp.float32, math.log(0.5), math.log(1.5)))
    position = jnp.arange(NX, dtype=jnp.float32)[None, None, :, None] / NX
    noise = jnp.clip(jax.random.normal(keys[2], shape, jnp.float32), -4.0, 4.0)
    ramp = jnp.exp(math.log(3.0) * position) / math.sqrt(3.0)
    return spread * ramp * rough * noise


def touch_ends(entries, stream_key, low, top_value):
    longest = entries.shape.index(max(entries.shape))
    spots = []
    for shift in (0, 1):
        where = [jax.random.randint(jax.random.fold_in(stream_key, axis), (), 0, length) for axis, length in enumerate(entries.shape)]
        where[longest] = (where[longest] + shift) % entries.shape[longest]
        spots.append(tuple(where))
    return entries.at[spots[0]].set(low).at[spots[1]].set(top_value)


def block_levels(key, dims, shards, smallest, top_value):
    gain, own = 1.0, jax.random.fold_in(key, 6)
    for dim, parts in shards:
        steps = jnp.exp(jax.random.uniform(jax.random.fold_in(own, dim), (parts,), jnp.float32, smallest / len(shards), top_value / len(shards)))
        gain = gain * jnp.repeat(steps, dims[dim] // parts).reshape([-1 if axis == dim else 1 for axis in range(len(dims))])
    return gain


def bell_draw(key, shape, scale, most, shards=(), held_as=jnp.bfloat16):
    result = scale * jax.random.normal(key, shape, jnp.float32)
    if shards:
        result = result * block_levels(key, shape, shards, -0.22, 0.18)
    return jnp.clip(result, -most, most).astype(held_as)


def setup_inputs(seed: int = 0) -> dict:
    streams_of = jax.random.split(jax.random.key(seed), 7)
    return {
        "particles": draw_particles(jax.random.fold_in(streams_of[6], 71), 0),
        "background": bell_draw(streams_of[1], (LAYERS, NX, NY), 1.0, 6.0, ((1, 128), (2, 2)), jnp.float32),
        "obs_tile": touch_ends(jax.random.randint(streams_of[2], (N_GX, N_GY * OBS_DEV), 0, TILES_DEV), jax.random.fold_in(streams_of[2], 1), 0, TILES_DEV - 1).astype(jnp.int32),
        "obs_mask": touch_ends((jax.random.randint(streams_of[3], (TILE * TILE, N_GX, N_GY * OBS_DEV), 0, 2) < 1).astype(jnp.int32), jax.random.fold_in(streams_of[3], 1), 0, 1),
        "obs_value": bell_draw(streams_of[4], (N_GX, N_GY * OBS_DEV), 1.0, 6.0, ((0, 128), (1, 2)), jnp.float32),
        "obs_var": jnp.clip(jnp.exp(math.log(1.0) - 2.3025851 * jax.random.uniform(streams_of[5], (N_GX, N_GY * OBS_DEV), jnp.float32) ** block_levels(streams_of[5], (N_GX, N_GY * OBS_DEV), ((0, 128), (1, 2)), -0.2, 0.2)), 0.1, 1.0),
    }


lap_weight = 0.25
prior_weight = 0.05
couple_weight = 0.5
step_length = 1.0
epsilon = 1e-06
highest = lax.Precision.HIGHEST

def laplace(field):
    total = jnp.roll(field, -1, -1) + jnp.roll(field, 1, -1)
    total = total + jnp.roll(field, -1, -2) + jnp.roll(field, 1, -2)
    return total - 4.0 * field

def prior_one(deviation):
    smooth = deviation - lap_weight * laplace(deviation)
    curved = smooth - lap_weight * laplace(smooth)
    return -prior_weight * (curved + couple_weight * (deviation - deviation[::-1]))

def reference(particles, background, obs_tile, obs_mask, obs_value, obs_var):
    tile_cols = CY // TILE
    block = jnp.arange(N_GX, dtype=jnp.int32)[:, None]
    column = jnp.arange(N_GY * OBS_DEV, dtype=jnp.int32)[None, :]
    offset = jnp.arange(TILE * TILE, dtype=jnp.int32)[:, None, None]
    rows = block * CX + obs_tile // tile_cols * TILE + offset // TILE
    cols = column // OBS_DEV * CY + obs_tile % tile_cols * TILE + offset % TILE
    weights = obs_mask.astype(jnp.float32)
    total_size = float(LAYERS * NX * NY)
    pair_count = float(NP * (NP - 1))
    off_diag = 1.0 - jnp.eye(NP, dtype=jnp.float32)
    state = particles
    for step in range(STEPS):
        deviation = state - background[None]
        prior_term = lax.map(prior_one, deviation)
        upper = state[:, 0]
        values = upper[:, rows, cols]
        mapped = 0.25 * lax.optimization_barrier(jnp.sum(weights[None] * values, axis=1))
        innovation = (obs_value[None] - mapped) / obs_var[None]
        contrib = (0.25 * weights)[None] * innovation[:, None]
        obs_upper = jnp.zeros((NP, NX, NY), jnp.float32).at[:, rows, cols].add(contrib)
        obs_term = jnp.stack([obs_upper, jnp.zeros_like(obs_upper)], axis=1)
        gradient = prior_term + obs_term
        flat_dev = deviation.reshape(NP, -1)
        flat_grad = gradient.reshape(NP, -1)
        gram = jnp.dot(flat_dev, flat_dev.T, precision=highest)
        diagonal = jnp.diagonal(gram)
        distance = diagonal[:, None] + diagonal[None, :] - 2.0 * gram
        width = jnp.sum(distance * off_diag) / (pair_count * total_size) + epsilon
        kernel = jnp.exp(-distance / (2.0 * width * total_size))
        attract = jnp.dot(kernel, flat_grad, precision=highest)
        pulled = jnp.dot(kernel, flat_dev, precision=highest)
        drift = (attract + (lax.optimization_barrier(jnp.sum(kernel, axis=1))[:, None] * flat_dev - pulled) / width) / NP
        scale = step_length / jnp.sqrt(jnp.sum(drift * drift) / (NP * total_size) + epsilon)
        state = state + scale * drift.reshape(state.shape)
    return state
```

```python
import functools

import jax
import jax.numpy as jnp
from jax import lax
from jax.experimental import pallas as pl
from jax.experimental.pallas import tpu as pltpu
from jax.sharding import Mesh
from jax.sharding import PartitionSpec as P

TILE = 4
LANES = 128
GX = ("gx_0", "gx_1", "gx_2", "gx_3")
AXES = GX + ("gy",)
NEAR = ("gx_2", "gx_3")
FAR = ("gx_0", "gx_1", "gy")

lap_weight = 0.25
prior_weight = 0.05
couple_weight = 0.5
epsilon = 1e-06
highest = lax.Precision.HIGHEST
f32 = jnp.float32
bf16 = jnp.bfloat16


def nn(a, b):
    return lax.dot_general(a, b, (((1,), (0,)), ((), ())), precision=highest, preferred_element_type=f32)


def nt(a, b):
    return lax.dot_general(a, b, (((1,), (1,)), ((), ())), precision=highest, preferred_element_type=f32)


def pieces(a):
    hi = a.astype(bf16)
    rest = a - hi.astype(f32)
    mid = rest.astype(bf16)
    return hi, mid, (rest - mid.astype(f32)).astype(bf16)


def dot_exact(a, table, dims):
    return sum(
        lax.dot_general(part, table, (dims, ((), ())), preferred_element_type=f32)
        for part in pieces(a)[::-1]
    )


def own_table(mask_row, tile, cols):
    pattern = jnp.concatenate(mask_row * (8 // TILE), axis=0)
    full = jnp.concatenate([pattern] * (cols // 8), axis=0)
    which = lax.broadcasted_iota(jnp.int32, (cols, LANES), 0).astype(jnp.int32) // TILE
    return jnp.where(which.astype(f32) == tile, full, 0.0).astype(bf16)


def edge_table(mask_row, tile, last_tile):
    pattern = jnp.concatenate(mask_row * (8 // TILE), axis=0)
    full = jnp.concatenate([pattern] * (LANES // 8), axis=0)
    lane = lax.broadcasted_iota(jnp.int32, (LANES, LANES), 0)
    which = jnp.where(lane < TILE, 0.0, jnp.where(lane >= LANES - TILE, last_tile, -1.0))
    return jnp.where(which == tile, full, 0.0).astype(bf16)


def pack_kernel(geom, part_ref, back_ref, tile_ref, mask_ref, value_ref, var_ref, main_ref, edge_ref):
    count, layers, rows, cols = geom
    tiles = cols // LANES
    per = layers * rows * tiles
    lane = lax.broadcasted_iota(jnp.int32, (count, LANES), 1)
    edge = jnp.zeros((count, LANES), f32)
    for l in range(layers):
        for r in range(rows):
            base = (l * rows + r) * 2 * TILE + TILE
            for ct in range(tiles):
                cell = part_ref[pl.ds((l * tiles + ct) * rows + r, count, stride=per), :]
                dev = cell - back_ref[l, r : r + 1, ct * LANES : (ct + 1) * LANES]
                main_ref[(l * rows + r) * count : (l * rows + r + 1) * count, ct * LANES : (ct + 1) * LANES] = dev
                if ct == 0:
                    rolled = pltpu.roll(dev, base, axis=1) if base else dev
                    edge = jnp.where((lane >= base) & (lane < base + TILE), rolled, edge)
                if ct == tiles - 1:
                    rolled = pltpu.roll(dev, base, axis=1)
                    edge = jnp.where((lane >= base - TILE) & (lane < base), rolled, edge)
    edge_ref[0:count, :] = edge
    tile = tile_ref[...].astype(f32)
    seen = jnp.zeros((8, LANES), f32)
    for r in range(rows):
        masks = [mask_ref[r * TILE + c].astype(f32) for c in range(TILE)]
        for c in range(TILE):
            edge_ref[count + r * TILE + c : count + r * TILE + c + 1, :] = masks[c]
        table = own_table(masks, tile, cols)
        field = jnp.broadcast_to(back_ref[0, r : r + 1, :], (8, cols))
        seen = seen + dot_exact(field, table, ((1,), (0,)))
    value = value_ref[...] - 0.25 * seen[0:1]
    base = count + rows * TILE
    edge_ref[base : base + 1, :] = tile
    edge_ref[base + 1 : base + 2, :] = value
    edge_ref[base + 2 : base + 3, :] = var_ref[...]
    edge_ref[base + 3 : base + 8, :] = jnp.zeros((5, LANES), f32)
    top = layers * rows * count
    main_ref[top : top + 8, :] = jnp.zeros((8, cols), f32)
    for k in range(rows * TILE + 3):
        main_ref[top + k // tiles : top + k // tiles + 1, (k % tiles) * LANES : (k % tiles + 1) * LANES] = edge_ref[
            count + k : count + k + 1, :
        ]


def stencil_kernel(
    geom,
    own_ref,
    low_ref,
    high_ref,
    side_ref,
    side_low_ref,
    side_high_ref,
    grad_ref,
    hess_ref,
    gram_ref,
    edges,
    grads,
    obs,
    obs_two,
):
    count, layers, rows, cols = geom
    tiles = cols // LANES
    top = layers * rows * count
    last_tile = float(cols // TILE - 1)
    mains = (low_ref, own_ref, high_ref)
    sides = (side_low_ref, side_ref, side_high_ref)
    for g in range(3):
        block = sides[g][0:count, :]
        for l in range(layers):
            for r in range(rows):
                base = (l * rows + r) * 2 * TILE + TILE
                edges[g, l, r] = pltpu.roll(block, LANES - base, axis=1)

    def obs_rows(g):
        def fetch(k):
            return mains[g][top + k // tiles : top + k // tiles + 1, (k % tiles) * LANES : (k % tiles + 1) * LANES]

        return fetch

    def side_rows(g):
        def fetch(k):
            return sides[g][count + k : count + k + 1, :]

        return fetch

    cells = rows * TILE
    wanted = {0: (rows - 2, rows - 1), 1: tuple(range(rows)), 2: (0, 1)}
    own_tables = None
    for g in range(3):
        fetch = obs_rows(g)
        tile, value, var = fetch(cells), fetch(cells + 1), fetch(cells + 2)
        tables = [own_table([fetch(r * TILE + c) for c in range(TILE)], tile, cols) for r in range(rows)]
        seen = sum(
            dot_exact(mains[g][r * count : (r + 1) * count, :], tables[r], ((1,), (0,))) for r in range(rows)
        )
        pull = (0.25 * value - 0.0625 * seen) / var
        for r in wanted[g]:
            obs[(g - 1) * rows + r + 2, :, 0:cols] = dot_exact(pull, tables[r], ((1,), (1,)))
        if g == 1:
            own_tables, own_var = tables, var
        fetch = side_rows(g)
        tile, value, var = fetch(cells), fetch(cells + 1), fetch(cells + 2)
        tables = [edge_table([fetch(r * TILE + c) for c in range(TILE)], tile, last_tile) for r in range(rows)]
        seen = sum(dot_exact(edges[g, 0, r], tables[r], ((1,), (0,))) for r in range(rows))
        pull = (0.25 * value - 0.0625 * seen) / var
        for r in wanted[g]:
            obs[(g - 1) * rows + r + 2, :, cols:] = dot_exact(pull, tables[r], ((1,), (1,)))

    wide = cols + LANES

    def smooth(mid, up, down):
        around = pltpu.roll(mid, 1, axis=1) + pltpu.roll(mid, wide - 1, axis=1) + up + down
        return 2.0 * mid - lap_weight * around

    def first(i, carry):
        ps = pl.multiple_of(i * 8, 8)

        def field(l, r):
            g, rr = divmod(r + rows, rows)
            start = pl.multiple_of((l * rows + rr) * count + ps, 8)
            return jnp.concatenate([mains[g][pl.ds(start, 8), :], edges[g, l, rr, pl.ds(ps, 8), :]], axis=1)

        for l in range(layers):
            level = [smooth(field(l, r), field(l, r - 1), field(l, r + 1)) for r in range(-3, rows + 3)]
            for r in range(-2, rows + 2):
                k = r + 3
                curved = smooth(level[k], level[k - 1], level[k + 1])
                out = -prior_weight * (curved + couple_weight * (field(l, r) - field(1 - l, r)))
                if l == 0:
                    out = out + obs[r + 2, pl.ds(ps, 8), :]
                grads[l, r + 2, pl.ds(ps, 8), :] = out
        return carry

    lax.fori_loop(0, count // 8, first, 0)
    seen = sum(dot_exact(grads[0, r + 2, :, 0:cols], own_tables[r], ((1,), (0,))) for r in range(rows))
    pull = -0.0625 * seen / own_var
    for r in range(rows):
        obs_two[r] = dot_exact(pull, own_tables[r], ((1,), (1,)))

    def second(i, carry):
        ps = pl.multiple_of(i * 8, 8)

        def field(l, r):
            return grads[l, r + 2, pl.ds(ps, 8), :]

        for l in range(layers):
            level = [smooth(field(l, r), field(l, r - 1), field(l, r + 1)) for r in range(-1, rows + 1)]
            for r in range(rows):
                k = r + 1
                mine = field(l, r)
                curved = smooth(level[k], level[k - 1], level[k + 1])
                out = -prior_weight * (curved + couple_weight * (mine - field(1 - l, r)))
                out = out[:, 0:cols]
                if l == 0:
                    out = out + obs_two[r, pl.ds(ps, 8), :]
                start = pl.multiple_of((l * rows + r) * count + ps, 8)
                hess_ref[pl.ds(start, 8), :] = out
                grad_ref[pl.ds(start, 8), :] = mine[:, 0:cols]
        return carry

    lax.fori_loop(0, count // 8, second, 0)
    total = jnp.zeros((3 * count, 3 * count), f32)
    for k in range(layers * rows):
        span = slice(k * count, (k + 1) * count)
        stack = jnp.concatenate([own_ref[span, :], grad_ref[span, :], hess_ref[span, :]], axis=0)
        total = total + nt(stack, stack)
    c = count
    gram_ref[0:c, 0:c] = total[0:c, 0:c]
    gram_ref[0:c, c:] = total[0:c, c : 2 * c]
    gram_ref[c : 2 * c, 0:c] = total[c : 2 * c, c : 2 * c]
    gram_ref[c : 2 * c, c:] = total[0:c, 2 * c :]
    gram_ref[2 * c :, 0:c] = total[c : 2 * c, 2 * c :]
    gram_ref[2 * c :, c:] = total[2 * c :, 2 * c :]


def mix_kernel(geom, total_size, gram_ref, own_ref, grad_ref, hess_ref, back_ref, out_ref):
    count, layers, rows, cols = geom
    tiles = cols // LANES
    per = layers * rows * tiles
    c = count
    dd, dg = gram_ref[0:c, 0:c], gram_ref[0:c, c:]
    gg, dh = gram_ref[c : 2 * c, 0:c], gram_ref[c : 2 * c, c:]
    gh, hh = gram_ref[2 * c :, 0:c], gram_ref[2 * c :, c:]
    row = lax.broadcasted_iota(jnp.int32, (c, c), 0)
    col = lax.broadcasted_iota(jnp.int32, (c, c), 1)
    eye = jnp.where(row == col, 1.0, 0.0)
    pair_count = float(c * (c - 1))

    def weights(gram):
        distance = (
            jnp.sum(gram * eye, axis=1, keepdims=True) + jnp.sum(gram * eye, axis=0, keepdims=True) - 2.0 * gram
        )
        width = jnp.sum(distance * (1.0 - eye), keepdims=True) / (pair_count * total_size) + epsilon
        kernel = jnp.exp(-distance / (2.0 * width * total_size))
        spread = (eye * jnp.sum(kernel, axis=1, keepdims=True) - kernel) / (width * c)
        return kernel / c, spread

    def inner(a, x, b):
        return jnp.sum(nn(a, x) * b, keepdims=True)

    def step_scale(square_sum):
        return 1.0 / jnp.sqrt(square_sum / (c * total_size) + epsilon)

    push, pull = weights(dd)
    dev_drift = nt(dd, pull) + nt(dg, push)
    drift_dev = nn(pull, dd) + nt(push, dg)
    grad_part = nn(pull, dg) + nn(push, gg)
    drift_drift = nt(nn(pull, dd) + nt(push, dg), pull) + nt(grad_part, push)
    scale = step_scale(jnp.sum(drift_drift * eye, keepdims=True))
    gram = dd + scale * (dev_drift + drift_dev) + scale * scale * drift_drift
    push_two, pull_two = weights(gram)
    keep = eye + scale * pull
    gain = scale * push
    on_dev = nn(pull_two, keep)
    on_grad = nn(push_two, keep) + nn(pull_two, gain)
    on_hess = nn(push_two, gain)
    square = (
        inner(on_dev, dd, on_dev)
        + inner(on_grad, gg, on_grad)
        + inner(on_hess, hh, on_hess)
        + 2.0 * (inner(on_dev, dg, on_grad) + inner(on_dev, dh, on_hess) + inner(on_grad, gh, on_hess))
    )
    scale_two = step_scale(square)
    mix = jnp.concatenate(
        [scale * pull + scale_two * on_dev, gain + scale_two * on_grad, scale_two * on_hess], axis=1
    )
    for l in range(layers):
        for r in range(rows):
            k = l * rows + r
            span = slice(k * c, (k + 1) * c)
            own = own_ref[span, :]
            stack = jnp.concatenate([own, grad_ref[span, :], hess_ref[span, :]], axis=0)
            new = own + back_ref[l, r : r + 1, :] + nn(mix, stack)
            for ct in range(tiles):
                out_ref[pl.ds((l * tiles + ct) * rows + r, c, stride=per), :] = new[:, ct * LANES : (ct + 1) * LANES]


def all_sum(part):
    near = 1
    for axis in NEAR:
        near *= lax.axis_size(axis)
    far = 1
    for axis in FAR:
        far *= lax.axis_size(axis)
    rows = part.shape[0]
    split = part.reshape(near, rows // near, part.shape[1])
    split = lax.all_to_all(split, NEAR, 0, 0, tiled=True)
    mine = jnp.sum(split, axis=0)
    mine = lax.all_to_all(jnp.broadcast_to(mine, (far,) + mine.shape), FAR, 0, 0, tiled=True)
    mine = jnp.sum(mine, axis=0)
    whole = lax.all_to_all(jnp.broadcast_to(mine, (near,) + mine.shape), NEAR, 0, 0, tiled=True)
    return whole.reshape(part.shape)


def shifted(count_x, count_y, step, flip):
    pairs = []
    for x in range(count_x):
        for y in range(count_y):
            target = (x + step) % count_x
            pairs.append((x * count_y + y, target * count_y + ((y + 1) % count_y if flip else y)))
    return pairs


def per_device(particles, background, obs_tile, obs_mask, obs_value, obs_var):
    geom = particles.shape
    count, layers, rows, cols = geom
    tiles = cols // LANES
    count_x, count_y = lax.axis_size(GX), lax.axis_size("gy")
    total_size = float(layers * rows * cols * count_x * count_y)
    flat = particles.reshape(count, layers, rows, tiles, LANES).transpose(0, 1, 3, 2, 4)
    flat = flat.reshape(count * layers * rows * tiles, LANES)
    block = layers * rows * count
    params = pltpu.CompilerParams(vmem_limit_bytes=24 * 1024 * 1024)
    main, edge = pl.pallas_call(
        functools.partial(pack_kernel, geom),
        out_shape=(
            jax.ShapeDtypeStruct((block + 8, cols), f32),
            jax.ShapeDtypeStruct((count + rows * TILE + 8, LANES), f32),
        ),
        compiler_params=params,
        name="pack",
    )(flat, background, obs_tile, obs_mask, obs_value, obs_var)
    low = lax.ppermute(main, AXES, shifted(count_x, count_y, 1, False))
    high = lax.ppermute(main, AXES, shifted(count_x, count_y, -1, False))
    side = lax.ppermute(edge, AXES, shifted(count_x, count_y, 0, True))
    side_low = lax.ppermute(edge, AXES, shifted(count_x, count_y, 1, True))
    side_high = lax.ppermute(edge, AXES, shifted(count_x, count_y, -1, True))
    grad, hess, gram = pl.pallas_call(
        functools.partial(stencil_kernel, geom),
        out_shape=(
            jax.ShapeDtypeStruct((block, cols), f32),
            jax.ShapeDtypeStruct((block, cols), f32),
            jax.ShapeDtypeStruct((3 * count, 2 * count), f32),
        ),
        scratch_shapes=[
            pltpu.VMEM((3, layers, rows, count, LANES), f32),
            pltpu.VMEM((layers, rows + 4, count, cols + LANES), f32),
            pltpu.VMEM((rows + 4, count, cols + LANES), f32),
            pltpu.VMEM((rows, count, cols), f32),
        ],
        compiler_params=params,
        name="stencil",
    )(main, low, high, side, side_low, side_high)
    gram = all_sum(gram)
    out = pl.pallas_call(
        functools.partial(mix_kernel, geom, total_size),
        out_shape=jax.ShapeDtypeStruct(flat.shape, f32),
        compiler_params=params,
        name="mix",
    )(gram, main, grad, hess, background)
    out = out.reshape(count, layers, tiles, rows, LANES).transpose(0, 1, 3, 2, 4)
    return out.reshape(geom)


def solution(mesh):
    count_x = mesh.shape["gx"]
    sizes = (4, 2, 8, 2) if count_x == 128 else (1, 1, count_x // 2, 2)
    finer = Mesh(mesh.devices.reshape(*sizes, mesh.shape["gy"]), AXES)
    in_specs = (
        P(None, None, GX, "gy"),
        P(None, GX, "gy"),
        P(GX, "gy"),
        P(None, GX, "gy"),
        P(GX, "gy"),
        P(GX, "gy"),
    )
    out_specs = P(None, None, GX, "gy")
    return jax.shard_map(per_device, mesh=finer, in_specs=in_specs, out_specs=out_specs, check_vma=False)
```

```python
import functools

import jax
import jax.numpy as jnp
from jax import lax
from jax.experimental import pallas as pl
from jax.experimental.pallas import tpu as pltpu
from jax.sharding import Mesh
from jax.sharding import PartitionSpec as P

TILE = 4
LANES = 128
GX = ("gx_0", "gx_1", "gx_2", "gx_3")
AXES = GX + ("gy",)
NEAR = ("gx_2", "gx_3")
FAR = ("gx_0", "gx_1", "gy")

lap_weight = 0.25
prior_weight = 0.05
couple_weight = 0.5
epsilon = 1e-06
highest = lax.Precision.HIGHEST
f32 = jnp.float32
bf16 = jnp.bfloat16


def nn(a, b):
    return lax.dot_general(a, b, (((1,), (0,)), ((), ())), precision=highest, preferred_element_type=f32)


def nt(a, b):
    return lax.dot_general(a, b, (((1,), (1,)), ((), ())), precision=highest, preferred_element_type=f32)


def pieces(a):
    hi = a.astype(bf16)
    rest = a - hi.astype(f32)
    mid = rest.astype(bf16)
    return hi, mid, (rest - mid.astype(f32)).astype(bf16)


def dot_exact(a, table, dims):
    return sum(
        lax.dot_general(part, table, (dims, ((), ())), preferred_element_type=f32)
        for part in pieces(a)[::-1]
    )


def own_table(mask_row, tile, cols):
    pattern = jnp.concatenate(mask_row * (8 // TILE), axis=0)
    full = jnp.concatenate([pattern] * (cols // 8), axis=0)
    which = lax.broadcasted_iota(jnp.int32, (cols, LANES), 0).astype(jnp.int32) // TILE
    return jnp.where(which.astype(f32) == tile, full, 0.0).astype(bf16)


def edge_table(mask_row, tile, last_tile):
    pattern = jnp.concatenate(mask_row * (8 // TILE), axis=0)
    full = jnp.concatenate([pattern] * (LANES // 8), axis=0)
    lane = lax.broadcasted_iota(jnp.int32, (LANES, LANES), 0)
    which = jnp.where(lane < TILE, 0.0, jnp.where(lane >= LANES - TILE, last_tile, -1.0))
    return jnp.where(which == tile, full, 0.0).astype(bf16)


def stored_row(ref, l, r, rows, flip):
    return jnp.where(flip == 1, ref[l, rows - 1 - r : rows - r, :], ref[l, r : r + 1, :])


def pack_kernel(
    geom, part_hbm, back_hbm, tile_hbm, mask_hbm, value_hbm, var_hbm, main_ref, edge_ref,
    part_ref, back_ref, tile_ref, mask_ref, value_ref, var_ref, sems,
):
    count, layers, rows, cols = geom
    tiles = cols // LANES
    per = layers * rows * tiles
    pairs = (
        (mask_hbm, mask_ref), (tile_hbm, tile_ref), (value_hbm, value_ref), (var_hbm, var_ref),
        (back_hbm, back_ref), (part_hbm, part_ref),
    )
    copies = [pltpu.make_async_copy(src, dst, sems.at[k]) for k, (src, dst) in enumerate(pairs)]
    for copy in copies:
        copy.start()
    flip = lax.axis_index("gx_3")
    lane = lax.broadcasted_iota(jnp.int32, (count, LANES), 1)
    for copy in copies[:5]:
        copy.wait()
    tile = tile_ref[...].astype(f32)
    seen = jnp.zeros((8, LANES), f32)
    for r in range(rows):
        source = r + flip * (rows - 1 - 2 * r)
        masks = [mask_ref[source * TILE + c].astype(f32) for c in range(TILE)]
        for c in range(TILE):
            edge_ref[count + r * TILE + c : count + r * TILE + c + 1, :] = masks[c]
        table = own_table(masks, tile, cols)
        field = jnp.broadcast_to(stored_row(back_ref, 0, r, rows, flip), (8, cols))
        seen = seen + dot_exact(field, table, ((1,), (0,)))
    value = value_ref[...] - 0.25 * seen[0:1]
    base = count + rows * TILE
    edge_ref[base : base + 1, :] = tile
    edge_ref[base + 1 : base + 2, :] = value
    edge_ref[base + 2 : base + 3, :] = var_ref[...]
    edge_ref[base + 3 : base + 8, :] = jnp.zeros((5, LANES), f32)
    top = layers * rows * count
    main_ref[top : top + 8, :] = jnp.zeros((8, cols), f32)
    for k in range(rows * TILE + 3):
        main_ref[top + k // tiles : top + k // tiles + 1, (k % tiles) * LANES : (k % tiles + 1) * LANES] = edge_ref[
            count + k : count + k + 1, :
        ]
    copies[5].wait()
    edge = jnp.zeros((count, LANES), f32)
    for l in range(layers):
        for r in range(rows):
            source = r + flip * (rows - 1 - 2 * r)
            base = (l * rows + r) * 2 * TILE + TILE
            back = stored_row(back_ref, l, r, rows, flip)
            for ct in range(tiles):
                cell = part_ref[pl.ds((l * tiles + ct) * rows + source, count, stride=per), :]
                dev = cell - back[:, ct * LANES : (ct + 1) * LANES]
                main_ref[(l * rows + r) * count : (l * rows + r + 1) * count, ct * LANES : (ct + 1) * LANES] = dev
                if ct == 0:
                    rolled = pltpu.roll(dev, base, axis=1)
                    edge = jnp.where((lane >= base) & (lane < base + TILE), rolled, edge)
                if ct == tiles - 1:
                    rolled = pltpu.roll(dev, base, axis=1)
                    edge = jnp.where((lane >= base - TILE) & (lane < base), rolled, edge)
    edge_ref[0:count, :] = edge


def fetch_main(geom, ref):
    count, layers, rows, cols = geom
    tiles, top = cols // LANES, layers * rows * count

    def fetch(k):
        return ref[top + k // tiles : top + k // tiles + 1, (k % tiles) * LANES : (k % tiles + 1) * LANES]

    return fetch


def masks_of(fetch, r):
    return [fetch(r * TILE + c) for c in range(TILE)]


def local_kernel(geom, own_ref, spread_ref, table_ref, square_ref):
    count, layers, rows, cols = geom
    fetch = fetch_main(geom, own_ref)
    cells = rows * TILE
    tile, value, var = fetch(cells), fetch(cells + 1), fetch(cells + 2)
    seen = jnp.zeros((count, LANES), f32)
    for r in range(rows):
        table = own_table(masks_of(fetch, r), tile, cols)
        table_ref[r * cols : (r + 1) * cols, :] = table
        seen = seen + dot_exact(own_ref[r * count : (r + 1) * count, :], table, ((1,), (0,)))
    pull = (0.25 * value - 0.0625 * seen) / var
    for r in range(rows):
        spread_ref[r * count : (r + 1) * count, :] = dot_exact(pull, table_ref[r * cols : (r + 1) * cols, :], ((1,), (1,)))
    total = jnp.zeros((count, count), f32)
    for k in range(layers * rows):
        block = own_ref[k * count : (k + 1) * count, :]
        total = total + nt(block, block)
    square_ref[...] = total


def stencil_kernel(
    geom,
    own_ref,
    high_ref,
    low_ref,
    side_ref,
    side_high_ref,
    side_low_ref,
    spread_ref,
    table_ref,
    square_ref,
    grad_ref,
    hess_ref,
    gram_ref,
    edges,
    grads,
    obs,
    obs_two,
):
    count, layers, rows, cols = geom
    last_tile = float(cols // TILE - 1)
    mains = (low_ref, own_ref, high_ref)
    sides = (side_low_ref, side_ref, side_high_ref)

    def place(r):
        if r < 0:
            return 0, -1 - r
        return (1, r) if r < rows else (2, 2 * rows - 1 - r)

    for g in range(3):
        block = sides[g][0:count, :]
        for l in range(layers):
            for r in range(rows):
                base = (l * rows + r) * 2 * TILE + TILE
                edges[g, l, r] = pltpu.roll(block, LANES - base, axis=1)

    cells = rows * TILE
    wanted = ((-1, -2), tuple(range(rows)), (rows, rows + 1))
    for g in range(3):
        if g != 1:
            fetch = fetch_main(geom, mains[g])
            tile, value, var = fetch(cells), fetch(cells + 1), fetch(cells + 2)
            tables = [own_table(masks_of(fetch, r), tile, cols) for r in range(rows)]
            seen = sum(
                dot_exact(mains[g][r * count : (r + 1) * count, :], tables[r], ((1,), (0,))) for r in range(rows)
            )
            pull = (0.25 * value - 0.0625 * seen) / var
            for r in wanted[g]:
                obs[r + 2, :, 0:cols] = dot_exact(pull, tables[place(r)[1]], ((1,), (1,)))
        fetch = lambda k: sides[g][count + k : count + k + 1, :]
        tile, value, var = fetch(cells), fetch(cells + 1), fetch(cells + 2)
        tables = [edge_table(masks_of(fetch, r), tile, last_tile) for r in range(rows)]
        seen = sum(dot_exact(edges[g, 0, r], tables[r], ((1,), (0,))) for r in range(rows))
        pull = (0.25 * value - 0.0625 * seen) / var
        for r in wanted[g]:
            obs[r + 2, :, cols:] = dot_exact(pull, tables[place(r)[1]], ((1,), (1,)))

    wide = cols + LANES

    def smooth(mid, up, down):
        around = pltpu.roll(mid, 1, axis=1) + pltpu.roll(mid, wide - 1, axis=1) + up + down
        return 2.0 * mid - lap_weight * around

    def first(i, carry):
        ps = pl.multiple_of(i * 8, 8)

        def field(l, r):
            g, rr = place(r)
            start = pl.multiple_of((l * rows + rr) * count + ps, 8)
            return jnp.concatenate([mains[g][pl.ds(start, 8), :], edges[g, l, rr, pl.ds(ps, 8), :]], axis=1)

        for l in range(layers):
            level = [smooth(field(l, r), field(l, r - 1), field(l, r + 1)) for r in range(-3, rows + 3)]
            for r in range(-2, rows + 2):
                k = r + 3
                curved = smooth(level[k], level[k - 1], level[k + 1])
                out = -prior_weight * (curved + couple_weight * (field(l, r) - field(1 - l, r)))
                if l == 0:
                    extra = obs[r + 2, pl.ds(ps, 8), :]
                    if 0 <= r < rows:
                        mine = spread_ref[pl.ds(pl.multiple_of(r * count + ps, 8), 8), :]
                        extra = jnp.concatenate([mine, extra[:, cols:]], axis=1)
                    out = out + extra
                grads[l, r + 2, pl.ds(ps, 8), :] = out
        return carry

    lax.fori_loop(0, count // 8, first, 0)
    table = lambda r: table_ref[r * cols : (r + 1) * cols, :]
    own_var = fetch_main(geom, own_ref)(cells + 2)
    seen = sum(dot_exact(grads[0, r + 2, :, 0:cols], table(r), ((1,), (0,))) for r in range(rows))
    pull = -0.0625 * seen / own_var
    for r in range(rows):
        obs_two[r] = dot_exact(pull, table(r), ((1,), (1,)))

    def second(i, carry):
        ps = pl.multiple_of(i * 8, 8)

        def field(l, r):
            return grads[l, r + 2, pl.ds(ps, 8), :]

        for l in range(layers):
            level = [smooth(field(l, r), field(l, r - 1), field(l, r + 1)) for r in range(-1, rows + 1)]
            for r in range(rows):
                k = r + 1
                mine = field(l, r)
                curved = smooth(level[k], level[k - 1], level[k + 1])
                out = -prior_weight * (curved + couple_weight * (mine - field(1 - l, r)))
                out = out[:, 0:cols]
                if l == 0:
                    out = out + obs_two[r, pl.ds(ps, 8), :]
                start = pl.multiple_of((l * rows + r) * count + ps, 8)
                hess_ref[pl.ds(start, 8), :] = out
                grad_ref[pl.ds(start, 8), :] = mine[:, 0:cols]
        return carry

    lax.fori_loop(0, count // 8, second, 0)
    total = jnp.zeros((2 * count, 3 * count), f32)
    for k in range(layers * rows):
        span = slice(k * count, (k + 1) * count)
        stack = jnp.concatenate([own_ref[span, :], grad_ref[span, :], hess_ref[span, :]], axis=0)
        total = total + nt(stack[count:], stack)
    c = count
    gram_ref[0:c, 0:c] = square_ref[...]
    gram_ref[0:c, c:] = total[0:c, 0:c]
    gram_ref[c : 2 * c, 0:c] = total[0:c, c : 2 * c]
    gram_ref[c : 2 * c, c:] = total[c:, 0:c]
    gram_ref[2 * c :, 0:c] = total[c:, c : 2 * c]
    gram_ref[2 * c :, c:] = total[c:, 2 * c :]


def mix_kernel(geom, total_size, gram_ref, own_ref, grad_ref, hess_ref, back_ref, out_ref):
    count, layers, rows, cols = geom
    tiles = cols // LANES
    per = layers * rows * tiles
    flip = lax.axis_index("gx_3")
    c = count
    dd, gd = gram_ref[0:c, 0:c], gram_ref[0:c, c:]
    gg, hd = gram_ref[c : 2 * c, 0:c], gram_ref[c : 2 * c, c:]
    hg, hh = gram_ref[2 * c :, 0:c], gram_ref[2 * c :, c:]
    row = lax.broadcasted_iota(jnp.int32, (c, c), 0)
    col = lax.broadcasted_iota(jnp.int32, (c, c), 1)
    eye = jnp.where(row == col, 1.0, 0.0)
    pair_count = float(c * (c - 1))

    def weights(gram):
        distance = (
            jnp.sum(gram * eye, axis=1, keepdims=True) + jnp.sum(gram * eye, axis=0, keepdims=True) - 2.0 * gram
        )
        width = jnp.sum(distance * (1.0 - eye), keepdims=True) / (pair_count * total_size) + epsilon
        kernel = jnp.exp(-distance / (2.0 * width * total_size))
        spread = (eye * jnp.sum(kernel, axis=1, keepdims=True) - kernel) / (width * c)
        return kernel / c, spread

    def inner(a, x, b):
        return jnp.sum(nn(a, x) * b, keepdims=True)

    def step_scale(square_sum):
        return 1.0 / jnp.sqrt(square_sum / (c * total_size) + epsilon)

    push, pull = weights(dd)
    drift_dev = nn(pull, dd) + nn(push, gd)
    drift_grad = nt(pull, gd) + nn(push, gg)
    drift_drift = nt(drift_dev, pull) + nt(drift_grad, push)
    dev_drift = drift_dev.T
    scale = step_scale(jnp.sum(drift_drift * eye, keepdims=True))
    gram = dd + scale * (dev_drift + drift_dev) + scale * scale * drift_drift
    push_two, pull_two = weights(gram)
    keep = eye + scale * pull
    gain = scale * push
    on_dev = nn(pull_two, keep)
    on_grad = nn(push_two, keep) + nn(pull_two, gain)
    on_hess = nn(push_two, gain)
    square = (
        inner(on_dev, dd, on_dev)
        + inner(on_grad, gg, on_grad)
        + inner(on_hess, hh, on_hess)
        + 2.0 * (inner(on_grad, gd, on_dev) + inner(on_hess, hd, on_dev) + inner(on_hess, hg, on_grad))
    )
    scale_two = step_scale(square)
    mix = jnp.concatenate(
        [scale * pull + scale_two * on_dev, gain + scale_two * on_grad, scale_two * on_hess], axis=1
    )
    for l in range(layers):
        for r in range(rows):
            k = l * rows + r
            span = slice(k * c, (k + 1) * c)
            source = r + flip * (rows - 1 - 2 * r)
            own = own_ref[span, :]
            stack = jnp.concatenate([own, grad_ref[span, :], hess_ref[span, :]], axis=0)
            new = own + stored_row(back_ref, l, r, rows, flip) + nn(mix, stack)
            for ct in range(tiles):
                out_ref[pl.ds((l * tiles + ct) * rows + source, c, stride=per), :] = new[:, ct * LANES : (ct + 1) * LANES]


def all_sum(part):
    near = 1
    for axis in NEAR:
        near *= lax.axis_size(axis)
    far = 1
    for axis in FAR:
        far *= lax.axis_size(axis)
    rows = part.shape[0]
    split = part.reshape(near, rows // near, part.shape[1])
    split = lax.all_to_all(split, NEAR, 0, 0, tiled=True)
    mine = jnp.sum(split, axis=0)
    mine = lax.all_to_all(jnp.broadcast_to(mine, (far,) + mine.shape), FAR, 0, 0, tiled=True)
    mine = jnp.sum(mine, axis=0)
    whole = lax.all_to_all(jnp.broadcast_to(mine, (near,) + mine.shape), NEAR, 0, 0, tiled=True)
    return whole.reshape(part.shape)


def swapped(count_x, count_y, pair, flip):
    pairs = []
    for x in range(count_x):
        step = 0 if pair is None else (1 if x % 2 == pair else -1)
        target = (x + step) % count_x
        for y in range(count_y):
            pairs.append((x * count_y + y, target * count_y + ((y + 1) % count_y if flip else y)))
    return pairs


def per_device(particles, background, obs_tile, obs_mask, obs_value, obs_var):
    geom = particles.shape
    count, layers, rows, cols = geom
    tiles = cols // LANES
    count_x, count_y = lax.axis_size(GX), lax.axis_size("gy")
    total_size = float(layers * rows * cols * count_x * count_y)
    flat = particles.reshape(count, layers, rows, tiles, LANES).transpose(0, 1, 3, 2, 4)
    flat = flat.reshape(count * layers * rows * tiles, LANES)
    block = layers * rows * count
    params = pltpu.CompilerParams(vmem_limit_bytes=24 * 1024 * 1024)
    inputs = (flat, background, obs_tile, obs_mask, obs_value, obs_var)
    main, edge = pl.pallas_call(
        functools.partial(pack_kernel, geom),
        out_shape=(
            jax.ShapeDtypeStruct((block + 8, cols), f32),
            jax.ShapeDtypeStruct((count + rows * TILE + 8, LANES), f32),
        ),
        in_specs=[pl.BlockSpec(memory_space=pltpu.HBM)] * len(inputs),
        scratch_shapes=[pltpu.VMEM(a.shape, a.dtype) for a in inputs] + [pltpu.SemaphoreType.DMA((len(inputs),))],
        compiler_params=params,
        name="pack",
    )(*[pltpu.with_memory_space_constraint(a, pltpu.HBM) for a in inputs])
    send = lambda what, pair, flip: lax.ppermute(what, AXES, swapped(count_x, count_y, pair, flip))
    side = send(edge, None, True)
    side_high = send(edge, 0, True)
    high = send(main, 0, False)
    side_low = send(edge, 1, True)
    low = send(main, 1, False)
    spread, table, square = pl.pallas_call(
        functools.partial(local_kernel, geom),
        out_shape=(
            jax.ShapeDtypeStruct((rows * count, cols), f32),
            jax.ShapeDtypeStruct((rows * cols, LANES), bf16),
            jax.ShapeDtypeStruct((count, count), f32),
        ),
        compiler_params=params,
        name="local",
    )(main)
    grad, hess, gram = pl.pallas_call(
        functools.partial(stencil_kernel, geom),
        out_shape=(
            jax.ShapeDtypeStruct((block, cols), f32),
            jax.ShapeDtypeStruct((block, cols), f32),
            jax.ShapeDtypeStruct((3 * count, 2 * count), f32),
        ),
        scratch_shapes=[
            pltpu.VMEM((3, layers, rows, count, LANES), f32),
            pltpu.VMEM((layers, rows + 4, count, cols + LANES), f32),
            pltpu.VMEM((rows + 4, count, cols + LANES), f32),
            pltpu.VMEM((rows, count, cols), f32),
        ],
        compiler_params=params,
        name="stencil",
    )(main, high, low, side, side_high, side_low, spread, table, square)
    gram = all_sum(gram)
    out = pl.pallas_call(
        functools.partial(mix_kernel, geom, total_size),
        out_shape=jax.ShapeDtypeStruct(flat.shape, f32),
        compiler_params=params,
        name="mix",
    )(gram, main, grad, hess, background)
    out = out.reshape(count, layers, tiles, rows, LANES).transpose(0, 1, 3, 2, 4)
    return out.reshape(geom)


def solution(mesh):
    count_x = mesh.shape["gx"]
    sizes = (4, 2, 8, 2) if count_x == 128 else (1, 1, count_x // 2, 2)
    finer = Mesh(mesh.devices.reshape(*sizes, mesh.shape["gy"]), AXES)
    in_specs = (
        P(None, None, GX, "gy"),
        P(None, GX, "gy"),
        P(GX, "gy"),
        P(None, GX, "gy"),
        P(GX, "gy"),
        P(GX, "gy"),
    )
    out_specs = P(None, None, GX, "gy")
    return jax.shard_map(per_device, mesh=finer, in_specs=in_specs, out_specs=out_specs, check_vma=False)
```

```python
import functools

import jax
import jax.numpy as jnp
from jax import lax
from jax.experimental import pallas as pl
from jax.experimental.pallas import tpu as pltpu
from jax.sharding import Mesh
from jax.sharding import PartitionSpec as P

TILE = 4
LANES = 128
GX = ("gx_0", "gx_1", "gx_2", "gx_3")
AXES = GX + ("gy",)

lap_weight = 0.25
prior_weight = 0.05
couple_weight = 0.5
epsilon = 1e-06
highest = lax.Precision.HIGHEST
f32 = jnp.float32
bf16 = jnp.bfloat16


def nn(a, b):
    return lax.dot_general(a, b, (((1,), (0,)), ((), ())), precision=highest, preferred_element_type=f32)


def nt(a, b):
    return lax.dot_general(a, b, (((1,), (1,)), ((), ())), precision=highest, preferred_element_type=f32)


def pieces(a):
    hi = a.astype(bf16)
    rest = a - hi.astype(f32)
    mid = rest.astype(bf16)
    return hi, mid, (rest - mid.astype(f32)).astype(bf16)


def dot_exact(a, table, dims):
    return sum(
        lax.dot_general(part, table, (dims, ((), ())), preferred_element_type=f32)
        for part in pieces(a)[::-1]
    )


def own_table(mask_row, tile, cols):
    pattern = jnp.concatenate(mask_row * (8 // TILE), axis=0)
    full = jnp.concatenate([pattern] * (cols // 8), axis=0)
    which = lax.broadcasted_iota(jnp.int32, (cols, LANES), 0).astype(jnp.int32) // TILE
    return jnp.where(which.astype(f32) == tile, full, 0.0).astype(bf16)


def edge_table(mask_row, tile, last_tile):
    pattern = jnp.concatenate(mask_row * (8 // TILE), axis=0)
    full = jnp.concatenate([pattern] * (LANES // 8), axis=0)
    lane = lax.broadcasted_iota(jnp.int32, (LANES, LANES), 0)
    which = jnp.where(lane < TILE, 0.0, jnp.where(lane >= LANES - TILE, last_tile, -1.0))
    return jnp.where(which == tile, full, 0.0).astype(bf16)


def stored_row(ref, l, r, rows, flip):
    return jnp.where(flip == 1, ref[l, rows - 1 - r : rows - r, :], ref[l, r : r + 1, :])


def pack_kernel(
    geom, part_hbm, back_hbm, tile_hbm, mask_hbm, value_hbm, var_hbm, main_ref, edge_ref, table_ref,
    part_ref, back_ref, tile_ref, mask_ref, value_ref, var_ref, sems,
):
    count, layers, rows, cols = geom
    tiles = cols // LANES
    per = layers * rows * tiles
    cells = rows * TILE
    pairs = (
        (mask_hbm, mask_ref), (tile_hbm, tile_ref), (value_hbm, value_ref), (var_hbm, var_ref),
        (back_hbm, back_ref), (part_hbm, part_ref),
    )
    copies = [pltpu.make_async_copy(src, dst, sems.at[k]) for k, (src, dst) in enumerate(pairs)]
    for copy in copies:
        copy.start()
    flip = lax.axis_index("gx_3")
    lane = lax.broadcasted_iota(jnp.int32, (count, LANES), 1)
    for copy in copies[:5]:
        copy.wait()
    tile = tile_ref[...].astype(f32)
    base = 2 * count
    top = layers * rows * count + count // tiles
    main_ref[top : top + 8, :] = jnp.zeros((8, cols), f32)
    edge_ref[base + cells : base + cells + 8, :] = jnp.zeros((8, LANES), f32)
    for r in range(rows):
        source = r + flip * (rows - 1 - 2 * r)
        masks = [mask_ref[source * TILE + c].astype(f32) for c in range(TILE)]
        for c in range(TILE):
            edge_ref[base + r * TILE + c : base + r * TILE + c + 1, :] = masks[c]
        table_ref[r * cols : (r + 1) * cols, :] = own_table(masks, tile, cols)
    edge_ref[base + cells : base + cells + 1, :] = tile
    edge_ref[base + cells + 1 : base + cells + 2, :] = var_ref[...]
    for k in range(cells + 2):
        main_ref[top + k // tiles : top + k // tiles + 1, (k % tiles) * LANES : (k % tiles + 1) * LANES] = edge_ref[
            base + k : base + k + 1, :
        ]
    copies[5].wait()
    edge = jnp.zeros((count, LANES), f32)
    seen = jnp.zeros((count, LANES), f32)
    for l in range(layers):
        for r in range(rows):
            source = r + flip * (rows - 1 - 2 * r)
            base = (l * rows + r) * 2 * TILE + TILE
            back = stored_row(back_ref, l, r, rows, flip)
            state = []
            for ct in range(tiles):
                cell = part_ref[pl.ds((l * tiles + ct) * rows + source, count, stride=per), :]
                state.append(cell)
                dev = cell - back[:, ct * LANES : (ct + 1) * LANES]
                main_ref[(l * rows + r) * count : (l * rows + r + 1) * count, ct * LANES : (ct + 1) * LANES] = dev
                if ct == 0:
                    rolled = pltpu.roll(dev, base, axis=1)
                    edge = jnp.where((lane >= base) & (lane < base + TILE), rolled, edge)
                if ct == tiles - 1:
                    rolled = pltpu.roll(dev, base, axis=1)
                    edge = jnp.where((lane >= base - TILE) & (lane < base), rolled, edge)
            if l == 0:
                table = table_ref[r * cols : (r + 1) * cols, :]
                seen = seen + dot_exact(jnp.concatenate(state, axis=1), table, ((1,), (0,)))
    edge_ref[0:count, :] = edge
    pull = (0.25 * value_ref[...] - 0.0625 * seen) / var_ref[...]
    edge_ref[count : 2 * count, :] = pull
    top = layers * rows * count
    part = count // tiles
    for ct in range(tiles):
        main_ref[top : top + part, ct * LANES : (ct + 1) * LANES] = pull[ct * part : (ct + 1) * part]


def fetch_main(geom, ref):
    count, layers, rows, cols = geom
    tiles = cols // LANES
    top = layers * rows * count + count // tiles

    def fetch(k):
        return ref[top + k // tiles : top + k // tiles + 1, (k % tiles) * LANES : (k % tiles + 1) * LANES]

    return fetch


def fetch_side(geom, ref):
    return lambda k: ref[2 * geom[0] + k : 2 * geom[0] + k + 1, :]


def pull_main(geom, ref):
    count, layers, rows, cols = geom
    top, tiles = layers * rows * count, cols // LANES
    part = count // tiles
    return jnp.concatenate([ref[top : top + part, ct * LANES : (ct + 1) * LANES] for ct in range(tiles)], axis=0)


def masks_of(fetch, r):
    return [fetch(r * TILE + c) for c in range(TILE)]


def local_kernel(geom, own_ref, table_ref, spread_ref, square_ref):
    count, layers, rows, cols = geom
    pull = pull_main(geom, own_ref)
    for r in range(rows):
        spread_ref[r * count : (r + 1) * count, :] = dot_exact(
            pull, table_ref[r * cols : (r + 1) * cols, :], ((1,), (1,))
        )
    total = jnp.zeros((count, count), f32)
    for k in range(layers * rows):
        block = own_ref[k * count : (k + 1) * count, :]
        total = total + nt(block, block)
    square_ref[...] = total


def unpack_edges(geom, side_ref, edges_ref):
    count, layers, rows, cols = geom
    block = side_ref[0:count, :]
    for l in range(layers):
        for r in range(rows):
            edges_ref[l, r] = pltpu.roll(block, LANES - ((l * rows + r) * 2 * TILE + TILE), axis=1)


def halo_spread(geom, main_ref, side_ref, wanted, obs):
    count, layers, rows, cols = geom
    cells = rows * TILE
    if main_ref is not None:
        fetch = fetch_main(geom, main_ref)
        pull, tile = pull_main(geom, main_ref), fetch(cells)
        for slot, r in wanted:
            obs[slot, :, 0:cols] = dot_exact(pull, own_table(masks_of(fetch, r), tile, cols), ((1,), (1,)))
    fetch = fetch_side(geom, side_ref)
    pull, tile = side_ref[count : 2 * count, :], fetch(cells)
    for slot, r in wanted:
        table = edge_table(masks_of(fetch, r), tile, float(cols // TILE - 1))
        obs[slot, :, cols:] = dot_exact(pull, table, ((1,), (1,)))


def smooth(mid, up, down):
    wide = mid.shape[1]
    return 8.0 * mid - (pltpu.roll(mid, 1, axis=1) + pltpu.roll(mid, wide - 1, axis=1) + up + down)


def prior_rows(layers, which, field, store):
    for l in range(layers):
        level = {}
        for r in which:
            for near in (r - 1, r, r + 1):
                if near not in level:
                    level[near] = smooth(field(l, near), field(l, near - 1), field(l, near + 1))
            mine = field(l, r)
            curved = smooth(level[r], level[r - 1], level[r + 1])
            store(l, r, mine, (-prior_weight / 16.0) * (curved + 16.0 * couple_weight * (mine - field(1 - l, r))))


def gradient_rows(geom, which, field, obs, spread_ref, store):
    count, layers, rows, cols = geom

    def step(i, carry):
        ps = pl.multiple_of(i * 8, 8)

        def put(l, r, mine, out):
            if l == 0:
                extra = obs[r - which[0], pl.ds(ps, 8), :]
                if 0 <= r < rows:
                    inner = spread_ref[pl.ds(pl.multiple_of(r * count + ps, 8), 8), :]
                    extra = jnp.concatenate([inner, extra[:, cols:]], axis=1)
                out = out + extra
            store(l, r, ps, out)

        prior_rows(layers, which, lambda l, r: field(l, r, ps), put)
        return carry

    lax.fori_loop(0, count // 8, step, 0)


def field_of(geom, own_ref, far_ref, own_edges, far_edges, far_row):
    count, layers, rows, cols = geom

    def field(l, r, ps):
        inside = 0 <= r < rows
        ref, edges, rr = (own_ref, own_edges, r) if inside else (far_ref, far_edges, far_row(r))
        start = pl.multiple_of((l * rows + rr) * count + ps, 8)
        return jnp.concatenate([ref[pl.ds(start, 8), :], edges[l, rr, pl.ds(ps, 8), :]], axis=1)

    return field


def upper_kernel(
    geom, own_ref, high_ref, side_ref, side_high_ref, spread_ref, up_ref, own_edges, far_edges, obs
):
    count, layers, rows, cols = geom
    which = tuple(range(rows - 2, rows + 2))
    far_row = lambda r: 2 * rows - 1 - r
    unpack_edges(geom, side_ref, own_edges)
    unpack_edges(geom, side_high_ref, far_edges)
    halo_spread(geom, None, side_ref, [(0, rows - 2), (1, rows - 1)], obs)
    halo_spread(geom, high_ref, side_high_ref, [(2, far_row(rows)), (3, far_row(rows + 1))], obs)

    def store(l, r, ps, out):
        start = pl.multiple_of((l * 4 + r - which[0]) * count + ps, 8)
        up_ref[pl.ds(start, 8), :] = out

    field = field_of(geom, own_ref, high_ref, own_edges, far_edges, far_row)
    gradient_rows(geom, which, field, obs, spread_ref, store)


def gram_terms(left, right):
    total = 0.0
    for i, j in ((2, 0), (0, 2), (1, 1), (1, 0), (0, 1), (0, 0)):
        total = total + lax.dot_general(left[i], right[j], (((1,), (1,)), ((), ())), preferred_element_type=f32)
    return total


def lower_kernel(
    geom, own_ref, low_ref, side_ref, side_low_ref, spread_ref, up_ref, table_ref, square_ref,
    grad_ref, hess_ref, mine_ref, other_ref, own_edges, far_edges, obs, grads, obs_two, full,
):
    count, layers, rows, cols = geom
    which = (-2, -1, 0, 1)
    far_row = lambda r: -1 - r
    unpack_edges(geom, side_ref, own_edges)
    unpack_edges(geom, side_low_ref, far_edges)
    halo_spread(geom, low_ref, side_low_ref, [(0, far_row(-2)), (1, far_row(-1))], obs)
    halo_spread(geom, None, side_ref, [(2, 0), (3, 1)], obs)

    def store(l, r, ps, out):
        grads[l, r + 2, pl.ds(ps, 8), :] = out

    field = field_of(geom, own_ref, low_ref, own_edges, far_edges, far_row)
    gradient_rows(geom, which, field, obs, spread_ref, store)

    def whole(l, r, ps, size):
        if r < 2:
            return grads[l, r + 2, pl.ds(ps, size), :]
        return up_ref[pl.ds(pl.multiple_of((l * 4 + r - rows + 2) * count + ps, 8), size), :]

    table = lambda r: table_ref[r * cols : (r + 1) * cols, :]
    seen = sum(dot_exact(whole(0, r, 0, count)[:, 0:cols], table(r), ((1,), (0,))) for r in range(rows))
    pull = -0.0625 * seen / fetch_main(geom, own_ref)(rows * TILE + 1)
    for r in range(rows):
        obs_two[r] = dot_exact(pull, table(r), ((1,), (1,)))

    def second(i, carry):
        ps = pl.multiple_of(i * 8, 8)

        def put(l, r, mine, out):
            out = out[:, 0:cols]
            if l == 0:
                out = out + obs_two[r, pl.ds(ps, 8), :]
            start = pl.multiple_of((l * rows + r) * count + ps, 8)
            hess_ref[pl.ds(start, 8), :] = out
            grad_ref[pl.ds(start, 8), :] = mine[:, 0:cols]

        prior_rows(layers, tuple(range(rows)), lambda l, r: whole(l, r, ps, 8), put)
        return carry

    lax.fori_loop(0, count // 8, second, 0)
    total = jnp.zeros((2 * count, 3 * count), f32)
    for k in range(layers * rows):
        span = slice(k * count, (k + 1) * count)
        stack = pieces(jnp.concatenate([own_ref[span, :], grad_ref[span, :], hess_ref[span, :]], axis=0))
        total = total + gram_terms([piece[count:] for piece in stack], stack)
    c = count
    row = lax.broadcasted_iota(jnp.int32, (c, c), 0)
    col = lax.broadcasted_iota(jnp.int32, (c, c), 1)
    eye = jnp.where(row == col, 1.0, 0.0)
    dd = square_ref[...]
    gd, gg = total[0:c, 0:c], total[0:c, c : 2 * c]
    hd, hg, hh = total[c:, 0:c], total[c:, c : 2 * c], total[c:, 2 * c :]
    full[...] = jnp.zeros(full.shape, f32)
    full[0:c, 0:c] = jnp.where(col >= row, dd, gg)
    full[0:c, c:] = jnp.where(col >= row, hh, hg)
    full[c : c + c // 2, 0:c] = gd[0 : c // 2]
    full[c : c + c // 2, c:] = gd[c // 2 :]
    top = c + c // 2
    full[top : top + 1, 0:c] = jnp.sum(gg * eye, axis=0, keepdims=True)
    full[top : top + 1, c:] = jnp.sum(hg * eye, axis=0, keepdims=True)
    full[top + 1 : top + 2, 0:c] = jnp.sum(hd[:, 0:1] * eye, axis=0, keepdims=True)
    flip = lax.axis_index("gx_3")
    half = full.shape[0] // 2
    mine_ref[...] = full[pl.ds(pl.multiple_of(flip * half, 8), half), :]
    other_ref[...] = full[pl.ds(pl.multiple_of((1 - flip) * half, 8), half), :]


def mix_kernel(
    geom, total_size, mine_ref, other_ref, own_ref, grad_ref, hess_ref, back_ref, out_ref, full
):
    count, layers, rows, cols = geom
    tiles = cols // LANES
    per = layers * rows * tiles
    flip = lax.axis_index("gx_3")
    c = count
    half = mine_ref.shape[0]
    full[pl.ds(pl.multiple_of(flip * half, 8), half), :] = mine_ref[...]
    full[pl.ds(pl.multiple_of((1 - flip) * half, 8), half), :] = other_ref[...]
    row = lax.broadcasted_iota(jnp.int32, (c, c), 0)
    col = lax.broadcasted_iota(jnp.int32, (c, c), 1)
    eye = jnp.where(row == col, 1.0, 0.0)
    pair_count = float(c * (c - 1))
    left, right = full[0:c, 0:c], full[0:c, c:]
    left_t, right_t = left.T, right.T
    top = c + c // 2
    dd = jnp.where(col >= row, left, left_t)
    hh = jnp.where(col >= row, right, right_t)
    gg = jnp.where(row > col, left, jnp.where(row < col, left_t, full[top : top + 1, 0:c]))
    hg = jnp.where(row > col, right, jnp.where(row < col, right_t, full[top : top + 1, c:]))
    gd = jnp.concatenate([full[c:top, 0:c], full[c:top, c:]], axis=0)
    hd_first = jnp.sum(eye * full[top + 1 : top + 2, 0:c], axis=1, keepdims=True)
    hd = gg - (gg[:, 0:1] - hd_first)

    def weights(gram):
        distance = (
            jnp.sum(gram * eye, axis=1, keepdims=True) + jnp.sum(gram * eye, axis=0, keepdims=True) - 2.0 * gram
        )
        width = jnp.sum(distance * (1.0 - eye), keepdims=True) / (pair_count * total_size) + epsilon
        kernel = jnp.exp(-distance / (2.0 * width * total_size))
        spread = (eye * jnp.sum(kernel, axis=1, keepdims=True) - kernel) / (width * c)
        return kernel / c, spread

    def step_scale(square_sum):
        return 1.0 / jnp.sqrt(square_sum / (c * total_size) + epsilon)

    push, pull = weights(dd)
    drift_dev = nn(pull, dd) + nn(push, gd)
    drift_grad = nt(pull, gd) + nn(push, gg)
    drift_drift = nt(drift_dev, pull) + nt(drift_grad, push)
    scale = step_scale(jnp.sum(drift_drift * eye, keepdims=True))
    gram = dd + scale * (drift_dev + drift_dev.T) + scale * scale * drift_drift
    push_two, pull_two = weights(gram)
    keep = eye + scale * pull
    gain = scale * push
    on_dev = nn(pull_two, keep)
    on_grad = nn(push_two, keep) + nn(pull_two, gain)
    on_hess = nn(push_two, gain)
    square = jnp.sum(
        nn(on_dev, dd) * on_dev
        + nn(on_grad, gg) * on_grad
        + nn(on_hess, hh) * on_hess
        + 2.0 * (nn(on_grad, gd) * on_dev + nn(on_hess, hd) * on_dev + nn(on_hess, hg) * on_grad),
        keepdims=True,
    )
    scale_two = step_scale(square)
    mix = jnp.concatenate(
        [scale * pull + scale_two * on_dev, gain + scale_two * on_grad, scale_two * on_hess], axis=1
    )
    mix = pieces(mix)
    lefts = (jnp.concatenate(mix, axis=0), jnp.concatenate(mix[:2], axis=0), mix[0])
    for l in range(layers):
        for r in range(rows):
            k = l * rows + r
            span = slice(k * c, (k + 1) * c)
            source = r + flip * (rows - 1 - 2 * r)
            own = own_ref[span, :]
            stack = pieces(jnp.concatenate([own, grad_ref[span, :], hess_ref[span, :]], axis=0))
            parts = [
                lax.dot_general(a, b, (((1,), (0,)), ((), ())), preferred_element_type=f32)
                for a, b in zip(lefts, stack)
            ]
            small = parts[0][2 * c :] + parts[1][c:] + parts[2]
            drift = (small + (parts[0][c : 2 * c] + parts[1][0:c])) + parts[0][0:c]
            new = own + stored_row(back_ref, l, r, rows, flip) + drift
            for ct in range(tiles):
                out_ref[pl.ds((l * tiles + ct) * rows + source, c, stride=per), :] = new[:, ct * LANES : (ct + 1) * LANES]


def all_sum(mine, other):
    swap = [(0, 1), (1, 0)]
    held = mine + lax.ppermute(other, "gx_3", swap)
    for axes in (("gx_2",), ("gx_0", "gx_1", "gy")):
        size = 1
        for axis in axes:
            size *= lax.axis_size(axis)
        copies = jnp.broadcast_to(held, (size,) + held.shape)
        held = jnp.sum(lax.all_to_all(copies, axes, 0, 0, tiled=True), axis=0)
    return held, lax.ppermute(held, "gx_3", swap)


def swapped(count_x, count_y, pair, flip):
    pairs = []
    for x in range(count_x):
        step = 0 if pair is None else (1 if x % 2 == pair else -1)
        target = (x + step) % count_x
        for y in range(count_y):
            pairs.append((x * count_y + y, target * count_y + ((y + 1) % count_y if flip else y)))
    return pairs


def per_device(particles, background, obs_tile, obs_mask, obs_value, obs_var):
    geom = particles.shape
    count, layers, rows, cols = geom
    tiles = cols // LANES
    count_x, count_y = lax.axis_size(GX), lax.axis_size("gy")
    total_size = float(layers * rows * cols * count_x * count_y)
    flat = particles.reshape(count, layers, rows, tiles, LANES).transpose(0, 1, 3, 2, 4)
    flat = flat.reshape(count * layers * rows * tiles, LANES)
    block = layers * rows * count
    params = pltpu.CompilerParams(vmem_limit_bytes=24 * 1024 * 1024)
    inputs = (flat, background, obs_tile, obs_mask, obs_value, obs_var)
    main, edge, table = pl.pallas_call(
        functools.partial(pack_kernel, geom),
        out_shape=(
            jax.ShapeDtypeStruct((block + count // tiles + 8, cols), f32),
            jax.ShapeDtypeStruct((2 * count + rows * TILE + 8, LANES), f32),
            jax.ShapeDtypeStruct((rows * cols, LANES), bf16),
        ),
        in_specs=[pl.BlockSpec(memory_space=pltpu.HBM)] * len(inputs),
        scratch_shapes=[pltpu.VMEM(a.shape, a.dtype) for a in inputs] + [pltpu.SemaphoreType.DMA((len(inputs),))],
        compiler_params=params,
        name="pack",
    )(*[pltpu.with_memory_space_constraint(a, pltpu.HBM) for a in inputs])
    send = lambda what, pair, flip: lax.ppermute(what, AXES, swapped(count_x, count_y, pair, flip))
    low = send(main, 1, False)
    side_low = send(edge, 1, True)
    high = send(main, 0, False)
    side_high = send(edge, 0, True)
    side = send(edge, None, True)
    spread, square = pl.pallas_call(
        functools.partial(local_kernel, geom),
        out_shape=(
            jax.ShapeDtypeStruct((rows * count, cols), f32),
            jax.ShapeDtypeStruct((count, count), f32),
        ),
        compiler_params=params,
        name="local",
    )(main, table)
    edges = pltpu.VMEM((layers, rows, count, LANES), f32)
    obs = pltpu.VMEM((4, count, cols + LANES), f32)
    up = pl.pallas_call(
        functools.partial(upper_kernel, geom),
        out_shape=jax.ShapeDtypeStruct((layers * 4 * count, cols + LANES), f32),
        scratch_shapes=[edges, edges, obs],
        compiler_params=params,
        name="upper",
    )(main, high, side, side_high, spread)
    full = pltpu.VMEM((7 * count // 4, LANES), f32)
    grad, hess, mine, other = pl.pallas_call(
        functools.partial(lower_kernel, geom),
        out_shape=(
            jax.ShapeDtypeStruct((block, cols), f32),
            jax.ShapeDtypeStruct((block, cols), f32),
            jax.ShapeDtypeStruct((7 * count // 8, LANES), f32),
            jax.ShapeDtypeStruct((7 * count // 8, LANES), f32),
        ),
        scratch_shapes=[
            edges,
            edges,
            obs,
            pltpu.VMEM((layers, 4, count, cols + LANES), f32),
            pltpu.VMEM((rows, count, cols), f32),
            full,
        ],
        compiler_params=params,
        name="lower",
    )(main, low, side, side_low, spread, up, table, square)
    mine, other = all_sum(mine, other)
    out = pl.pallas_call(
        functools.partial(mix_kernel, geom, total_size),
        out_shape=jax.ShapeDtypeStruct(flat.shape, f32),
        scratch_shapes=[full],
        compiler_params=params,
        name="mix",
    )(mine, other, main, grad, hess, background)
    out = out.reshape(count, layers, tiles, rows, LANES).transpose(0, 1, 3, 2, 4)
    return out.reshape(geom)


def solution(mesh):
    count_x = mesh.shape["gx"]
    sizes = (4, 2, 8, 2) if count_x == 128 else (1, 1, count_x // 2, 2)
    finer = Mesh(mesh.devices.reshape(*sizes, mesh.shape["gy"]), AXES)
    in_specs = (
        P(None, None, GX, "gy"),
        P(None, GX, "gy"),
        P(GX, "gy"),
        P(None, GX, "gy"),
        P(GX, "gy"),
        P(GX, "gy"),
    )
    out_specs = P(None, None, GX, "gy")
    return jax.shard_map(per_device, mesh=finer, in_specs=in_specs, out_specs=out_specs, check_vma=False)
```

```python
import functools

import jax
import jax.numpy as jnp
from jax import lax
from jax.experimental import pallas as pl
from jax.experimental.pallas import tpu as pltpu
from jax.sharding import Mesh
from jax.sharding import PartitionSpec as P

TILE = 4
LANES = 128
GX = ("gx_0", "gx_1", "gx_2", "gx_3")
AXES = GX + ("gy",)

prior_weight = 0.05
couple_weight = 0.5
epsilon = 1e-06
highest = lax.Precision.HIGHEST
f32 = jnp.float32
bf16 = jnp.bfloat16


def nn(a, b):
    return lax.dot_general(a, b, (((1,), (0,)), ((), ())), precision=highest, preferred_element_type=f32)


def nt(a, b):
    return lax.dot_general(a, b, (((1,), (1,)), ((), ())), precision=highest, preferred_element_type=f32)


def pieces(a):
    hi = a.astype(bf16)
    rest = a - hi.astype(f32)
    mid = rest.astype(bf16)
    return hi, mid, (rest - mid.astype(f32)).astype(bf16)


def dot_exact(a, table, dims):
    return sum(
        lax.dot_general(part, table, (dims, ((), ())), preferred_element_type=f32)
        for part in pieces(a)[::-1]
    )


def own_table(mask_row, tile, cols):
    pattern = jnp.concatenate(mask_row * (8 // TILE), axis=0)
    full = jnp.concatenate([pattern] * (cols // 8), axis=0)
    which = lax.broadcasted_iota(jnp.int32, (cols, LANES), 0).astype(jnp.int32) // TILE
    return jnp.where(which.astype(f32) == tile, full, 0.0).astype(bf16)


def stored_row(ref, l, r, rows, flip):
    return jnp.where(flip == 1, ref[l, rows - 1 - r : rows - r, :], ref[l, r : r + 1, :])


def pack_kernel(
    geom, part_hbm, back_hbm, tile_hbm, mask_hbm, value_hbm, var_hbm, main_ref, edge_ref, table_ref,
    part_ref, back_ref, tile_ref, mask_ref, value_ref, var_ref, sems,
):
    count, layers, rows, cols = geom
    tiles = cols // LANES
    per = layers * rows * tiles
    pairs = (
        (mask_hbm, mask_ref), (tile_hbm, tile_ref), (value_hbm, value_ref), (var_hbm, var_ref),
        (back_hbm, back_ref), (part_hbm, part_ref),
    )
    copies = [pltpu.make_async_copy(src, dst, sems.at[k]) for k, (src, dst) in enumerate(pairs)]
    for copy in copies:
        copy.start()
    flip = lax.axis_index("gx_3")
    lane = lax.broadcasted_iota(jnp.int32, (count, LANES), 1)
    for copy in copies[:5]:
        copy.wait()
    tile = tile_ref[...].astype(f32)
    top = layers * rows * count + count // tiles
    main_ref[top : top + 8, :] = jnp.zeros((8, cols), f32)
    facts = []
    for r in range(rows):
        source = r + flip * (rows - 1 - 2 * r)
        masks = [mask_ref[source * TILE + c].astype(f32) for c in range(TILE)]
        facts += masks
        table_ref[r * cols : (r + 1) * cols, :] = own_table(masks, tile, cols)
    for k, fact in enumerate(facts + [tile, var_ref[...]]):
        main_ref[top + k // tiles : top + k // tiles + 1, (k % tiles) * LANES : (k % tiles + 1) * LANES] = fact
    copies[5].wait()
    edge = jnp.zeros((count, LANES), f32)
    seen = jnp.zeros((count, LANES), f32)
    for l in range(layers):
        for r in range(rows):
            source = r + flip * (rows - 1 - 2 * r)
            base = (l * rows + r) * 2 * TILE + TILE
            back = stored_row(back_ref, l, r, rows, flip)
            state = []
            for ct in range(tiles):
                cell = part_ref[pl.ds((l * tiles + ct) * rows + source, count, stride=per), :]
                state.append(cell)
                dev = cell - back[:, ct * LANES : (ct + 1) * LANES]
                main_ref[(l * rows + r) * count : (l * rows + r + 1) * count, ct * LANES : (ct + 1) * LANES] = dev
                if ct == 0:
                    rolled = pltpu.roll(dev, base, axis=1)
                    edge = jnp.where((lane >= base) & (lane < base + TILE), rolled, edge)
                if ct == tiles - 1:
                    rolled = pltpu.roll(dev, base, axis=1)
                    edge = jnp.where((lane >= base - TILE) & (lane < base), rolled, edge)
            if l == 0:
                table = table_ref[r * cols : (r + 1) * cols, :]
                seen = seen + dot_exact(jnp.concatenate(state, axis=1), table, ((1,), (0,)))
    pull = (0.25 * value_ref[...] - 0.0625 * seen) / var_ref[...]
    for r in range(rows):
        base = (layers * rows + r) * 2 * TILE + TILE
        for start, low in ((0, base), (cols - LANES, base - TILE)):
            table = table_ref[r * cols + start : r * cols + start + LANES, :]
            rolled = pltpu.roll(dot_exact(pull, table, ((1,), (1,))), base, axis=1)
            edge = jnp.where((lane >= low) & (lane < low + TILE), rolled, edge)
    edge_ref[...] = edge
    top = layers * rows * count
    part = count // tiles
    for ct in range(tiles):
        main_ref[top : top + part, ct * LANES : (ct + 1) * LANES] = pull[ct * part : (ct + 1) * part]


def fetch_main(geom, ref):
    count, layers, rows, cols = geom
    tiles = cols // LANES
    top = layers * rows * count + count // tiles

    def fetch(k):
        return ref[top + k // tiles : top + k // tiles + 1, (k % tiles) * LANES : (k % tiles + 1) * LANES]

    return fetch


def pull_main(geom, ref):
    count, layers, rows, cols = geom
    top, tiles = layers * rows * count, cols // LANES
    part = count // tiles
    return jnp.concatenate([ref[top : top + part, ct * LANES : (ct + 1) * LANES] for ct in range(tiles)], axis=0)


def masks_of(fetch, r):
    return [fetch(r * TILE + c) for c in range(TILE)]


def rows_dot(left, right):
    return lax.dot_general(left, right, (((1,), (1,)), ((), ())), preferred_element_type=f32)


def gram_self(parts):
    hi, mid, lo = (part[...] for part in parts)
    cross = rows_dot(hi, lo)
    total = rows_dot(mid, mid) + (cross + cross.T)
    cross = rows_dot(hi, mid)
    return total + (cross + cross.T) + rows_dot(hi, hi)


def gram_cross(left, right):
    total = 0.0
    for i, j in ((2, 0), (0, 2), (1, 1), (1, 0), (0, 1), (0, 0)):
        total = total + rows_dot(left[i][...], right[j][...])
    return total


def local_kernel(geom, own_ref, table_ref, spread_ref, square_ref, *dev_refs):
    count, layers, rows, cols = geom
    pull = pull_main(geom, own_ref)
    for r in range(rows):
        spread_ref[r * count : (r + 1) * count, :] = dot_exact(
            pull, table_ref[r * cols : (r + 1) * cols, :], ((1,), (1,))
        )
    for k in range(layers * rows):
        for ref, piece in zip(dev_refs, pieces(own_ref[k * count : (k + 1) * count, :])):
            ref[:, k * cols : (k + 1) * cols] = piece
    square_ref[...] = gram_self(dev_refs)


def edge_tile(side_ref, slot):
    return pltpu.roll(side_ref[...], LANES - (slot * 2 * TILE + TILE), axis=1)


def smooth(mid, up, down):
    wide = mid.shape[1]
    return 8.0 * mid - (pltpu.roll(mid, 1, axis=1) + pltpu.roll(mid, wide - 1, axis=1) + up + down)


def prior_rows(layers, which, field, store):
    for l in range(layers):
        level = {}
        for r in which:
            for near in (r - 1, r, r + 1):
                if near not in level:
                    level[near] = smooth(field(l, near), field(l, near - 1), field(l, near + 1))
            mine = field(l, r)
            curved = smooth(level[r], level[r - 1], level[r + 1])
            store(l, r, mine, (-prior_weight / 16.0) * (curved + 16.0 * couple_weight * (mine - field(1 - l, r))))


def gradient_rows(geom, which, own_ref, far_ref, side_ref, side_far_ref, far_row, spread_ref, out_ref):
    count, layers, rows, cols = geom
    far_pull, far_fetch = pull_main(geom, far_ref), fetch_main(geom, far_ref)

    def row_of(r):
        return (own_ref, side_ref, r) if 0 <= r < rows else (far_ref, side_far_ref, far_row(r))

    def field(l, r):
        ref, side, rr = row_of(r)
        start = (l * rows + rr) * count
        return jnp.concatenate([ref[start : start + count, :], edge_tile(side, l * rows + rr)], axis=1)

    def put(l, r, mine, out):
        if l == 0:
            _, side, rr = row_of(r)
            if 0 <= r < rows:
                inner = spread_ref[r * count : (r + 1) * count, :]
            else:
                table = own_table(masks_of(far_fetch, rr), far_fetch(rows * TILE), cols)
                inner = dot_exact(far_pull, table, ((1,), (1,)))
            out = out + jnp.concatenate([inner, edge_tile(side, layers * rows + rr)], axis=1)
        start = (l * len(which) + r - which[0]) * count
        out_ref[start : start + count, :] = out

    prior_rows(layers, which, field, put)


def upper_kernel(geom, own_ref, high_ref, side_ref, side_high_ref, spread_ref, up_ref):
    rows = geom[2]
    which = tuple(range(rows - 2, rows + 2))
    far_row = lambda r: 2 * rows - 1 - r
    gradient_rows(geom, which, own_ref, high_ref, side_ref, side_high_ref, far_row, spread_ref, up_ref)


def lower_kernel(
    geom, own_ref, low_ref, side_ref, side_low_ref, spread_ref, up_ref, table_ref, square_ref,
    dev_hi, dev_mid, dev_lo, grad_ref, hess_ref, mine_ref, other_ref, hi_ref, mid_ref, lo_ref, down, full,
):
    count, layers, rows, cols = geom
    far_row = lambda r: -1 - r
    gradient_rows(geom, (-2, -1, 0, 1), own_ref, low_ref, side_ref, side_low_ref, far_row, spread_ref, down)

    def whole(l, r):
        ref, slot = (down, r + 2) if r < 2 else (up_ref, r - rows + 2)
        start = (l * 4 + slot) * count
        return ref[start : start + count, :]

    table = lambda r: table_ref[r * cols : (r + 1) * cols, :]
    seen = sum(dot_exact(whole(0, r)[:, 0:cols], table(r), ((1,), (0,))) for r in range(rows))
    pull = -0.0625 * seen / fetch_main(geom, own_ref)(rows * TILE + 1)
    parts = (hi_ref, mid_ref, lo_ref)

    def put(l, r, mine, out):
        out = out[:, 0:cols]
        if l == 0:
            out = out + dot_exact(pull, table(r), ((1,), (1,)))
        k = l * rows + r
        grad_ref[k * count : (k + 1) * count, :] = mine[:, 0:cols]
        hess_ref[k * count : (k + 1) * count, :] = out
        span = slice(k * cols, (k + 1) * cols)
        for ref, grad, hess in zip(parts, pieces(mine[:, 0:cols]), pieces(out)):
            ref[0:count, span] = grad
            ref[count:, span] = hess

    prior_rows(layers, tuple(range(rows)), whole, put)
    with_dev = gram_cross(parts, (dev_hi, dev_mid, dev_lo))
    total = gram_self(parts)
    c = count
    row = lax.broadcasted_iota(jnp.int32, (c, c), 0)
    col = lax.broadcasted_iota(jnp.int32, (c, c), 1)
    eye = jnp.where(row == col, 1.0, 0.0)
    dd = square_ref[...]
    gd, hd = with_dev[0:c], with_dev[c:]
    gg, hg, hh = total[0:c, 0:c], total[c:, 0:c], total[c:, c:]
    full[...] = jnp.zeros(full.shape, f32)
    full[0:c, 0:c] = jnp.where(col >= row, dd, gg)
    full[0:c, c:] = jnp.where(col >= row, hh, hg)
    full[c : c + c // 2, 0:c] = gd[0 : c // 2]
    full[c : c + c // 2, c:] = gd[c // 2 :]
    top = c + c // 2
    full[top : top + 1, 0:c] = jnp.sum(gg * eye, axis=0, keepdims=True)
    full[top : top + 1, c:] = jnp.sum(hg * eye, axis=0, keepdims=True)
    full[top + 1 : top + 2, 0:c] = jnp.sum(hd[:, 0:1] * eye, axis=0, keepdims=True)
    flip = lax.axis_index("gx_3")
    half = full.shape[0] // 2
    mine_ref[...] = full[pl.ds(pl.multiple_of(flip * half, 8), half), :]
    other_ref[...] = full[pl.ds(pl.multiple_of((1 - flip) * half, 8), half), :]


def mix_kernel(
    geom, total_size, mine_ref, other_ref, own_ref, grad_ref, hess_ref, back_ref, out_ref, full
):
    count, layers, rows, cols = geom
    tiles = cols // LANES
    per = layers * rows * tiles
    flip = lax.axis_index("gx_3")
    c = count
    half = mine_ref.shape[0]
    full[pl.ds(pl.multiple_of(flip * half, 8), half), :] = mine_ref[...]
    full[pl.ds(pl.multiple_of((1 - flip) * half, 8), half), :] = other_ref[...]
    row = lax.broadcasted_iota(jnp.int32, (c, c), 0)
    col = lax.broadcasted_iota(jnp.int32, (c, c), 1)
    eye = jnp.where(row == col, 1.0, 0.0)
    pair_count = float(c * (c - 1))
    left, right = full[0:c, 0:c], full[0:c, c:]
    left_t, right_t = left.T, right.T
    top = c + c // 2
    dd = jnp.where(col >= row, left, left_t)
    hh = jnp.where(col >= row, right, right_t)
    gg = jnp.where(row > col, left, jnp.where(row < col, left_t, full[top : top + 1, 0:c]))
    hg = jnp.where(row > col, right, jnp.where(row < col, right_t, full[top : top + 1, c:]))
    gd = jnp.concatenate([full[c:top, 0:c], full[c:top, c:]], axis=0)
    hd_first = jnp.sum(eye * full[top + 1 : top + 2, 0:c], axis=1, keepdims=True)
    hd = gg - (gg[:, 0:1] - hd_first)

    def weights(gram):
        distance = (
            jnp.sum(gram * eye, axis=1, keepdims=True) + jnp.sum(gram * eye, axis=0, keepdims=True) - 2.0 * gram
        )
        width = jnp.sum(distance * (1.0 - eye), keepdims=True) / (pair_count * total_size) + epsilon
        kernel = jnp.exp(-distance / (2.0 * width * total_size))
        spread = (eye * jnp.sum(kernel, axis=1, keepdims=True) - kernel) / (width * c)
        return kernel / c, spread

    def step_scale(square_sum):
        return 1.0 / jnp.sqrt(square_sum / (c * total_size) + epsilon)

    push, pull = weights(dd)
    drift_dev = nn(pull, dd) + nn(push, gd)
    drift_grad = nt(pull, gd) + nn(push, gg)
    drift_drift = nt(drift_dev, pull) + nt(drift_grad, push)
    scale = step_scale(jnp.sum(drift_drift * eye, keepdims=True))
    gram = dd + scale * (drift_dev + drift_dev.T) + scale * scale * drift_drift
    push_two, pull_two = weights(gram)
    keep = eye + scale * pull
    gain = scale * push
    on_dev = nn(pull_two, keep)
    on_grad = nn(push_two, keep) + nn(pull_two, gain)
    on_hess = nn(push_two, gain)
    square = jnp.sum(
        nn(on_dev, dd) * on_dev
        + nn(on_grad, gg) * on_grad
        + nn(on_hess, hh) * on_hess
        + 2.0 * (nn(on_grad, gd) * on_dev + nn(on_hess, hd) * on_dev + nn(on_hess, hg) * on_grad),
        keepdims=True,
    )
    scale_two = step_scale(square)
    mix = jnp.concatenate(
        [scale * pull + scale_two * on_dev, gain + scale_two * on_grad, scale_two * on_hess], axis=1
    )
    mix = pieces(mix)
    lefts = (jnp.concatenate(mix, axis=0), jnp.concatenate(mix[:2], axis=0), mix[0])
    for l in range(layers):
        for r in range(rows):
            k = l * rows + r
            span = slice(k * c, (k + 1) * c)
            source = r + flip * (rows - 1 - 2 * r)
            own = own_ref[span, :]
            stack = pieces(jnp.concatenate([own, grad_ref[span, :], hess_ref[span, :]], axis=0))
            parts = [
                lax.dot_general(a, b, (((1,), (0,)), ((), ())), preferred_element_type=f32)
                for a, b in zip(lefts, stack)
            ]
            small = parts[0][2 * c :] + parts[1][c:] + parts[2]
            drift = (small + (parts[0][c : 2 * c] + parts[1][0:c])) + parts[0][0:c]
            new = own + stored_row(back_ref, l, r, rows, flip) + drift
            for ct in range(tiles):
                out_ref[pl.ds((l * tiles + ct) * rows + source, c, stride=per), :] = new[:, ct * LANES : (ct + 1) * LANES]


def all_sum(mine, other):
    swap = [(0, 1), (1, 0)]
    held = mine + lax.ppermute(other, "gx_3", swap)
    for axes in (("gx_2",), ("gx_0", "gx_1", "gy")):
        size = 1
        for axis in axes:
            size *= lax.axis_size(axis)
        copies = jnp.broadcast_to(held, (size,) + held.shape)
        held = jnp.sum(lax.all_to_all(copies, axes, 0, 0, tiled=True), axis=0)
    return held, lax.ppermute(held, "gx_3", swap)


def swapped(count_x, count_y, pair, flip):
    pairs = []
    for x in range(count_x):
        step = 0 if pair is None else (1 if x % 2 == pair else -1)
        target = (x + step) % count_x
        for y in range(count_y):
            pairs.append((x * count_y + y, target * count_y + ((y + 1) % count_y if flip else y)))
    return pairs


def per_device(particles, background, obs_tile, obs_mask, obs_value, obs_var):
    geom = particles.shape
    count, layers, rows, cols = geom
    tiles = cols // LANES
    count_x, count_y = lax.axis_size(GX), lax.axis_size("gy")
    total_size = float(layers * rows * cols * count_x * count_y)
    flat = particles.reshape(count, layers, rows, tiles, LANES).transpose(0, 1, 3, 2, 4)
    flat = flat.reshape(count * layers * rows * tiles, LANES)
    block = layers * rows * count
    params = pltpu.CompilerParams(vmem_limit_bytes=24 * 1024 * 1024)
    inputs = (flat, background, obs_tile, obs_mask, obs_value, obs_var)
    main, edge, table = pl.pallas_call(
        functools.partial(pack_kernel, geom),
        out_shape=(
            jax.ShapeDtypeStruct((block + count // tiles + 8, cols), f32),
            jax.ShapeDtypeStruct((count, LANES), f32),
            jax.ShapeDtypeStruct((rows * cols, LANES), bf16),
        ),
        in_specs=[pl.BlockSpec(memory_space=pltpu.HBM)] * len(inputs),
        scratch_shapes=[pltpu.VMEM(a.shape, a.dtype) for a in inputs] + [pltpu.SemaphoreType.DMA((len(inputs),))],
        compiler_params=params,
        name="pack",
    )(*[pltpu.with_memory_space_constraint(a, pltpu.HBM) for a in inputs])

    def send(what, pair, flip):
        return lax.ppermute(what, AXES, swapped(count_x, count_y, pair, flip))

    side = send(edge, None, True)
    low = send(main, 1, False)
    high = send(main, 0, False)
    side_low = send(side, 1, False)
    side_high = send(side, 0, False)
    half = jax.ShapeDtypeStruct((count, block // count * cols), bf16)
    spread, square, *dev = pl.pallas_call(
        functools.partial(local_kernel, geom),
        out_shape=(
            jax.ShapeDtypeStruct((rows * count, cols), f32),
            jax.ShapeDtypeStruct((count, count), f32),
        )
        + (half,) * 3,
        compiler_params=params,
        name="local",
    )(main, table)
    up = pl.pallas_call(
        functools.partial(upper_kernel, geom),
        out_shape=jax.ShapeDtypeStruct((layers * 4 * count, cols + LANES), f32),
        compiler_params=params,
        name="upper",
    )(main, high, side, side_high, spread)
    full = pltpu.VMEM((7 * count // 4, LANES), f32)
    grad, hess, mine, other = pl.pallas_call(
        functools.partial(lower_kernel, geom),
        out_shape=(jax.ShapeDtypeStruct((block, cols), f32),) * 2
        + (jax.ShapeDtypeStruct((7 * count // 8, LANES), f32),) * 2,
        scratch_shapes=[pltpu.VMEM((2 * count, half.shape[1]), bf16)] * 3
        + [pltpu.VMEM((layers * 4 * count, cols + LANES), f32), full],
        compiler_params=params,
        name="lower",
    )(main, low, side, side_low, spread, up, table, square, *dev)
    mine, other = all_sum(mine, other)
    out = pl.pallas_call(
        functools.partial(mix_kernel, geom, total_size),
        out_shape=jax.ShapeDtypeStruct(flat.shape, f32),
        scratch_shapes=[full],
        compiler_params=params,
        name="mix",
    )(mine, other, main, grad, hess, background)
    out = out.reshape(count, layers, tiles, rows, LANES).transpose(0, 1, 3, 2, 4)
    return out.reshape(geom)


def solution(mesh):
    count_x = mesh.shape["gx"]
    sizes = (4, 2, 8, 2) if count_x == 128 else (1, 1, count_x // 2, 2)
    finer = Mesh(mesh.devices.reshape(*sizes, mesh.shape["gy"]), AXES)
    in_specs = (
        P(None, None, GX, "gy"),
        P(None, GX, "gy"),
        P(GX, "gy"),
        P(None, GX, "gy"),
        P(GX, "gy"),
        P(GX, "gy"),
    )
    out_specs = P(None, None, GX, "gy")
    return jax.shard_map(per_device, mesh=finer, in_specs=in_specs, out_specs=out_specs, check_vma=False)
```

```python
import functools

import jax
import jax.numpy as jnp
from jax import lax
from jax.experimental import pallas as pl
from jax.experimental.pallas import tpu as pltpu
from jax.sharding import Mesh
from jax.sharding import PartitionSpec as P

TILE = 4
HALF = TILE // 2
LANES = 128
GX = ("gx_0", "gx_1", "gx_2", "gx_3")
AXES = GX + ("gy",)

prior_weight = 0.05
couple_weight = 0.5
epsilon = 1e-06
highest = lax.Precision.HIGHEST
f32 = jnp.float32
bf16 = jnp.bfloat16


def nn(a, b):
    return lax.dot_general(a, b, (((1,), (0,)), ((), ())), precision=highest, preferred_element_type=f32)


def nt(a, b):
    return lax.dot_general(a, b, (((1,), (1,)), ((), ())), precision=highest, preferred_element_type=f32)


def pieces(a):
    hi = a.astype(bf16)
    rest = a - hi.astype(f32)
    mid = rest.astype(bf16)
    return hi, mid, (rest - mid.astype(f32)).astype(bf16)


def dot_exact(a, table, dims):
    return sum(
        lax.dot_general(part, table, (dims, ((), ())), preferred_element_type=f32)
        for part in pieces(a)[::-1]
    )


def own_table(mask_row, tile, cols):
    pattern = jnp.concatenate(mask_row * (8 // TILE), axis=0)
    full = jnp.concatenate([pattern] * (cols // 8), axis=0)
    which = lax.broadcasted_iota(jnp.int32, (cols, LANES), 0).astype(jnp.int32) // TILE
    return jnp.where(which.astype(f32) == tile, full, 0.0).astype(bf16)


def stored_row(ref, l, r, rows, flip):
    return jnp.where(flip == 1, ref[l, rows - 1 - r : rows - r, :], ref[l, r : r + 1, :])


def pack_kernel(
    geom, part_hbm, back_hbm, tile_hbm, mask_hbm, value_hbm, var_hbm, near_ref, far_ref, edge_ref, table_ref,
    part_ref, back_ref, tile_ref, mask_ref, value_ref, var_ref, sems,
):
    count, layers, rows, cols = geom
    tiles = cols // LANES
    per = layers * rows * tiles
    pairs = (
        (mask_hbm, mask_ref), (tile_hbm, tile_ref), (value_hbm, value_ref), (var_hbm, var_ref),
        (back_hbm, back_ref), (part_hbm, part_ref),
    )
    copies = [pltpu.make_async_copy(src, dst, sems.at[k]) for k, (src, dst) in enumerate(pairs)]
    for copy in copies:
        copy.start()
    flip = lax.axis_index("gx_3")
    lane = lax.broadcasted_iota(jnp.int32, (count, LANES), 1)
    for copy in copies[:5]:
        copy.wait()
    tile = tile_ref[...].astype(f32)
    top = layers * HALF * count + count // tiles
    far_ref[top : top + 8, :] = jnp.zeros((8, cols), f32)
    facts = []
    for r in range(rows):
        source = r + flip * (rows - 1 - 2 * r)
        masks = [mask_ref[source * TILE + c].astype(f32) for c in range(TILE)]
        facts += masks
        table_ref[r * cols : (r + 1) * cols, :] = own_table(masks, tile, cols)
    for k, fact in enumerate(facts + [tile, var_ref[...]]):
        far_ref[top + k // tiles : top + k // tiles + 1, (k % tiles) * LANES : (k % tiles + 1) * LANES] = fact
    copies[5].wait()
    edge = jnp.zeros((count, LANES), f32)
    seen = jnp.zeros((count, LANES), f32)
    for l in range(layers):
        for r in range(rows):
            source = r + flip * (rows - 1 - 2 * r)
            base = (l * rows + r) * 2 * TILE + TILE
            back = stored_row(back_ref, l, r, rows, flip)
            half_ref, start = (near_ref, far_ref)[r // HALF], (l * HALF + r % HALF) * count
            state = []
            for ct in range(tiles):
                cell = part_ref[pl.ds((l * tiles + ct) * rows + source, count, stride=per), :]
                state.append(cell)
                dev = cell - back[:, ct * LANES : (ct + 1) * LANES]
                half_ref[start : start + count, ct * LANES : (ct + 1) * LANES] = dev
                if ct == 0:
                    rolled = pltpu.roll(dev, base, axis=1)
                    edge = jnp.where((lane >= base) & (lane < base + TILE), rolled, edge)
                if ct == tiles - 1:
                    rolled = pltpu.roll(dev, base, axis=1)
                    edge = jnp.where((lane >= base - TILE) & (lane < base), rolled, edge)
            if l == 0:
                table = table_ref[r * cols : (r + 1) * cols, :]
                seen = seen + dot_exact(jnp.concatenate(state, axis=1), table, ((1,), (0,)))
    pull = (0.25 * value_ref[...] - 0.0625 * seen) / var_ref[...]
    for r in range(rows):
        base = (layers * rows + r) * 2 * TILE + TILE
        for start, low in ((0, base), (cols - LANES, base - TILE)):
            table = table_ref[r * cols + start : r * cols + start + LANES, :]
            rolled = pltpu.roll(dot_exact(pull, table, ((1,), (1,))), base, axis=1)
            edge = jnp.where((lane >= low) & (lane < low + TILE), rolled, edge)
    edge_ref[...] = edge
    top = layers * HALF * count
    part = count // tiles
    for ct in range(tiles):
        far_ref[top : top + part, ct * LANES : (ct + 1) * LANES] = pull[ct * part : (ct + 1) * part]


def fetch_main(geom, ref):
    count, layers, _, cols = geom
    tiles = cols // LANES
    top = layers * HALF * count + count // tiles

    def fetch(k):
        return ref[top + k // tiles : top + k // tiles + 1, (k % tiles) * LANES : (k % tiles + 1) * LANES]

    return fetch


def pull_main(geom, ref):
    count, layers, _, cols = geom
    top, tiles = layers * HALF * count, cols // LANES
    part = count // tiles
    return jnp.concatenate([ref[top : top + part, ct * LANES : (ct + 1) * LANES] for ct in range(tiles)], axis=0)


def masks_of(fetch, r):
    return [fetch(r * TILE + c) for c in range(TILE)]


def rows_dot(left, right):
    return lax.dot_general(left, right, (((1,), (1,)), ((), ())), preferred_element_type=f32)


def gram_self(parts):
    hi, mid, lo = (part[...] for part in parts)
    cross = rows_dot(hi, lo)
    total = rows_dot(mid, mid) + (cross + cross.T)
    cross = rows_dot(hi, mid)
    return total + (cross + cross.T) + rows_dot(hi, hi)


def gram_cross(left, right):
    total = 0.0
    for i, j in ((2, 0), (0, 2), (1, 1), (1, 0), (0, 1), (0, 0)):
        total = total + rows_dot(left[i][...], right[j][...])
    return total


def slab_row(halves, count, l, r):
    start = (l * HALF + r % HALF) * count
    return halves[r // HALF][start : start + count, :]


def local_kernel(geom, near_ref, far_ref, table_ref, spread_ref, square_ref, *dev_refs):
    count, layers, rows, cols = geom
    pull = pull_main(geom, far_ref)
    for r in range(rows):
        spread_ref[r * count : (r + 1) * count, :] = dot_exact(
            pull, table_ref[r * cols : (r + 1) * cols, :], ((1,), (1,))
        )
    for l in range(layers):
        for r in range(rows):
            k = l * HALF + r % HALF
            half = dev_refs[3 * (r // HALF) : 3 * (r // HALF) + 3]
            for ref, piece in zip(half, pieces(slab_row((near_ref, far_ref), count, l, r))):
                ref[:, k * cols : (k + 1) * cols] = piece
    square_ref[...] = gram_self(dev_refs[:3]) + gram_self(dev_refs[3:])


def edge_tile(side_ref, slot):
    return pltpu.roll(side_ref[...], LANES - (slot * 2 * TILE + TILE), axis=1)


def smooth(mid, up, down):
    wide = mid.shape[1]
    return 8.0 * mid - (pltpu.roll(mid, 1, axis=1) + pltpu.roll(mid, wide - 1, axis=1) + up + down)


def prior_rows(layers, which, field, store):
    for l in range(layers):
        level = {}
        for r in which:
            for near in (r - 1, r, r + 1):
                if near not in level:
                    level[near] = smooth(field(l, near), field(l, near - 1), field(l, near + 1))
            mine = field(l, r)
            curved = smooth(level[r], level[r - 1], level[r + 1])
            store(l, r, mine, (-prior_weight / 16.0) * (curved + 16.0 * couple_weight * (mine - field(1 - l, r))))


def gradient_rows(geom, which, own, other, side_ref, side_other_ref, other_row, spread_ref, out_ref):
    count, layers, rows, cols = geom

    def row_of(r):
        return (own, side_ref, r) if 0 <= r < rows else (other, side_other_ref, other_row(r))

    def field(l, r):
        halves, side, rr = row_of(r)
        return jnp.concatenate([slab_row(halves, count, l, rr), edge_tile(side, l * rows + rr)], axis=1)

    def put(l, r, mine, out):
        if l == 0:
            halves, side, rr = row_of(r)
            if 0 <= r < rows:
                inner = spread_ref[r * count : (r + 1) * count, :]
            else:
                fetch = fetch_main(geom, halves[1])
                table = own_table(masks_of(fetch, rr), fetch(rows * TILE), cols)
                inner = dot_exact(pull_main(geom, halves[1]), table, ((1,), (1,)))
            out = out + jnp.concatenate([inner, edge_tile(side, layers * rows + rr)], axis=1)
        start = (l * len(which) + r - which[0]) * count
        out_ref[start : start + count, :] = out

    prior_rows(layers, which, field, put)


def upper_kernel(
    geom, near_ref, far_ref, high_near_ref, high_far_ref, side_ref, side_high_ref, spread_ref, up_ref
):
    rows = geom[2]
    which = tuple(range(rows - 2, rows + 2))
    own, other = (near_ref, far_ref), (high_near_ref, high_far_ref)
    other_row = lambda r: 2 * rows - 1 - r
    gradient_rows(geom, which, own, other, side_ref, side_high_ref, other_row, spread_ref, up_ref)


def gradient_at(count, l, r, down_ref, mid_ref, up_ref):
    if r < 0:
        ref, start = down_ref, (l * 2 + r + 2) * count
    elif r < 2:
        ref, start = mid_ref, (l * 2 + r) * count
    else:
        ref, start = up_ref, (l * 4 + r - 2) * count
    return ref[start : start + count, :]


def linear_rows(geom, which, field, extra, hess_ref, parts):
    count, layers, _, cols = geom

    def put(l, r, mine, out):
        out = out[:, 0:cols]
        if l == 0:
            out = out + extra(r)
        k = l * HALF + r % HALF
        hess_ref[k * count : (k + 1) * count, :] = out
        span = slice(k * cols, (k + 1) * cols)
        for ref, grad, hess in zip(parts, pieces(mine[:, 0:cols]), pieces(out)):
            ref[0:count, span] = grad
            ref[count:, span] = hess

    prior_rows(layers, which, field, put)


def middle_kernel(
    geom, near_ref, far_ref, low_near_ref, side_ref, side_low_ref, spread_ref, up_ref, table_ref,
    dev_hi, dev_mid, dev_lo, mid_ref, grad_near_ref, grad_far_ref, hess_ref, spread_two_ref, with_dev_ref, self_ref,
    *parts,
):
    count, layers, rows, cols = geom
    own = (near_ref, far_ref)
    other_row = lambda r: -1 - r
    gradient_rows(geom, (0, 1), own, (low_near_ref, None), side_ref, side_low_ref, other_row, spread_ref, mid_ref)
    field = lambda l, r: gradient_at(count, l, r, None, mid_ref, up_ref)
    for l in range(layers):
        for r in range(rows):
            start = (l * HALF + r % HALF) * count
            (grad_near_ref, grad_far_ref)[r // HALF][start : start + count, :] = field(l, r)[:, 0:cols]
    table = lambda r: table_ref[r * cols : (r + 1) * cols, :]
    seen = sum(dot_exact(field(0, r)[:, 0:cols], table(r), ((1,), (0,))) for r in range(rows))
    pull = -0.0625 * seen / fetch_main(geom, far_ref)(rows * TILE + 1)
    for r in range(HALF):
        spread_two_ref[r * count : (r + 1) * count, :] = dot_exact(pull, table(r), ((1,), (1,)))
    extra = lambda r: dot_exact(pull, table(r), ((1,), (1,)))
    linear_rows(geom, (2, 3), field, extra, hess_ref, parts)
    with_dev_ref[...] = gram_cross(parts, (dev_hi, dev_mid, dev_lo))
    self_ref[...] = gram_self(parts)


def lower_kernel(
    geom, near_ref, far_ref, low_near_ref, low_far_ref, side_ref, side_low_ref, mid_ref, up_ref, spread_two_ref,
    square_ref, with_dev_ref, self_ref, dev_hi, dev_mid, dev_lo, hess_ref, mine_ref, other_ref,
    hi_ref, mid_part_ref, lo_ref, down, full,
):
    count, _, _, _ = geom
    own, other = (near_ref, far_ref), (low_near_ref, low_far_ref)
    other_row = lambda r: -1 - r
    gradient_rows(geom, (-2, -1), own, other, side_ref, side_low_ref, other_row, None, down)
    field = lambda l, r: gradient_at(count, l, r, down, mid_ref, up_ref)
    extra = lambda r: spread_two_ref[r * count : (r + 1) * count, :]
    parts = (hi_ref, mid_part_ref, lo_ref)
    linear_rows(geom, (0, 1), field, extra, hess_ref, parts)
    with_dev = gram_cross(parts, (dev_hi, dev_mid, dev_lo)) + with_dev_ref[...]
    total = gram_self(parts) + self_ref[...]
    c = count
    row = lax.broadcasted_iota(jnp.int32, (c, c), 0)
    col = lax.broadcasted_iota(jnp.int32, (c, c), 1)
    eye = jnp.where(row == col, 1.0, 0.0)
    dd = square_ref[...]
    gd, hd = with_dev[0:c], with_dev[c:]
    gg, hg, hh = total[0:c, 0:c], total[c:, 0:c], total[c:, c:]
    full[...] = jnp.zeros(full.shape, f32)
    full[0:c, 0:c] = jnp.where(col >= row, dd, gg)
    full[0:c, c:] = jnp.where(col >= row, hh, hg)
    full[c : c + c // 2, 0:c] = gd[0 : c // 2]
    full[c : c + c // 2, c:] = gd[c // 2 :]
    top = c + c // 2
    full[top : top + 1, 0:c] = jnp.sum(gg * eye, axis=0, keepdims=True)
    full[top : top + 1, c:] = jnp.sum(hg * eye, axis=0, keepdims=True)
    full[top + 1 : top + 2, 0:c] = jnp.sum(hd[:, 0:1] * eye, axis=0, keepdims=True)
    flip = lax.axis_index("gx_3")
    half = full.shape[0] // 2
    mine_ref[...] = full[pl.ds(pl.multiple_of(flip * half, 8), half), :]
    other_ref[...] = full[pl.ds(pl.multiple_of((1 - flip) * half, 8), half), :]


def mix_kernel(
    geom, total_size, mine_ref, other_ref, near_ref, far_ref, grad_near_ref, grad_far_ref, hess_near_ref, hess_far_ref,
    back_ref, out_ref, full,
):
    count, layers, rows, cols = geom
    tiles = cols // LANES
    per = layers * rows * tiles
    flip = lax.axis_index("gx_3")
    c = count
    half = mine_ref.shape[0]
    full[pl.ds(pl.multiple_of(flip * half, 8), half), :] = mine_ref[...]
    full[pl.ds(pl.multiple_of((1 - flip) * half, 8), half), :] = other_ref[...]
    row = lax.broadcasted_iota(jnp.int32, (c, c), 0)
    col = lax.broadcasted_iota(jnp.int32, (c, c), 1)
    eye = jnp.where(row == col, 1.0, 0.0)
    pair_count = float(c * (c - 1))
    left, right = full[0:c, 0:c], full[0:c, c:]
    left_t, right_t = left.T, right.T
    top = c + c // 2
    dd = jnp.where(col >= row, left, left_t)
    hh = jnp.where(col >= row, right, right_t)
    gg = jnp.where(row > col, left, jnp.where(row < col, left_t, full[top : top + 1, 0:c]))
    hg = jnp.where(row > col, right, jnp.where(row < col, right_t, full[top : top + 1, c:]))
    gd = jnp.concatenate([full[c:top, 0:c], full[c:top, c:]], axis=0)
    hd_first = jnp.sum(eye * full[top + 1 : top + 2, 0:c], axis=1, keepdims=True)
    hd = gg - (gg[:, 0:1] - hd_first)

    def weights(gram):
        distance = (
            jnp.sum(gram * eye, axis=1, keepdims=True) + jnp.sum(gram * eye, axis=0, keepdims=True) - 2.0 * gram
        )
        width = jnp.sum(distance * (1.0 - eye), keepdims=True) / (pair_count * total_size) + epsilon
        kernel = jnp.exp(-distance / (2.0 * width * total_size))
        spread = (eye * jnp.sum(kernel, axis=1, keepdims=True) - kernel) / (width * c)
        return kernel / c, spread

    def step_scale(square_sum):
        return 1.0 / jnp.sqrt(square_sum / (c * total_size) + epsilon)

    push, pull = weights(dd)
    drift_dev = nn(pull, dd) + nn(push, gd)
    drift_grad = nt(pull, gd) + nn(push, gg)
    drift_drift = nt(drift_dev, pull) + nt(drift_grad, push)
    scale = step_scale(jnp.sum(drift_drift * eye, keepdims=True))
    gram = dd + scale * (drift_dev + drift_dev.T) + scale * scale * drift_drift
    push_two, pull_two = weights(gram)
    keep = eye + scale * pull
    gain = scale * push
    on_dev = nn(pull_two, keep)
    on_grad = nn(push_two, keep) + nn(pull_two, gain)
    on_hess = nn(push_two, gain)
    square = jnp.sum(
        nn(on_dev, dd) * on_dev
        + nn(on_grad, gg) * on_grad
        + nn(on_hess, hh) * on_hess
        + 2.0 * (nn(on_grad, gd) * on_dev + nn(on_hess, hd) * on_dev + nn(on_hess, hg) * on_grad),
        keepdims=True,
    )
    scale_two = step_scale(square)
    mix = jnp.concatenate(
        [scale * pull + scale_two * on_dev, gain + scale_two * on_grad, scale_two * on_hess], axis=1
    )
    mix = pieces(mix)
    lefts = (jnp.concatenate(mix, axis=0), jnp.concatenate(mix[:2], axis=0), mix[0])
    for l in range(layers):
        for r in range(rows):
            source = r + flip * (rows - 1 - 2 * r)
            own = slab_row((near_ref, far_ref), c, l, r)
            grad = slab_row((grad_near_ref, grad_far_ref), c, l, r)
            hess = slab_row((hess_near_ref, hess_far_ref), c, l, r)
            stack = pieces(jnp.concatenate([own, grad, hess], axis=0))
            parts = [
                lax.dot_general(a, b, (((1,), (0,)), ((), ())), preferred_element_type=f32)
                for a, b in zip(lefts, stack)
            ]
            small = parts[0][2 * c :] + parts[1][c:] + parts[2]
            drift = (small + (parts[0][c : 2 * c] + parts[1][0:c])) + parts[0][0:c]
            new = own + stored_row(back_ref, l, r, rows, flip) + drift
            for ct in range(tiles):
                out_ref[pl.ds((l * tiles + ct) * rows + source, c, stride=per), :] = new[:, ct * LANES : (ct + 1) * LANES]


def all_sum(mine, other):
    swap = [(0, 1), (1, 0)]
    held = mine + lax.ppermute(other, "gx_3", swap)
    for axes in (("gx_2",), ("gx_0", "gx_1", "gy")):
        size = 1
        for axis in axes:
            size *= lax.axis_size(axis)
        copies = jnp.broadcast_to(held, (size,) + held.shape)
        held = jnp.sum(lax.all_to_all(copies, axes, 0, 0, tiled=True), axis=0)
    return held, lax.ppermute(held, "gx_3", swap)


def swapped(count_x, count_y, pair, flip):
    pairs = []
    for x in range(count_x):
        step = 0 if pair is None else (1 if x % 2 == pair else -1)
        target = (x + step) % count_x
        for y in range(count_y):
            pairs.append((x * count_y + y, target * count_y + ((y + 1) % count_y if flip else y)))
    return pairs


def per_device(particles, background, obs_tile, obs_mask, obs_value, obs_var):
    geom = particles.shape
    count, layers, rows, cols = geom
    tiles = cols // LANES
    count_x, count_y = lax.axis_size(GX), lax.axis_size("gy")
    total_size = float(layers * rows * cols * count_x * count_y)
    flat = particles.reshape(count, layers, rows, tiles, LANES).transpose(0, 1, 3, 2, 4)
    flat = flat.reshape(count * layers * rows * tiles, LANES)
    half = layers * HALF * count
    wide = cols + LANES
    params = pltpu.CompilerParams(vmem_limit_bytes=24 * 1024 * 1024)
    shape = jax.ShapeDtypeStruct
    inputs = (flat, background, obs_tile, obs_mask, obs_value, obs_var)
    near, far, edge, table = pl.pallas_call(
        functools.partial(pack_kernel, geom),
        out_shape=(
            shape((half, cols), f32),
            shape((half + count // tiles + 8, cols), f32),
            shape((count, LANES), f32),
            shape((rows * cols, LANES), bf16),
        ),
        in_specs=[pl.BlockSpec(memory_space=pltpu.HBM)] * len(inputs),
        scratch_shapes=[pltpu.VMEM(a.shape, a.dtype) for a in inputs] + [pltpu.SemaphoreType.DMA((len(inputs),))],
        compiler_params=params,
        name="pack",
    )(*[pltpu.with_memory_space_constraint(a, pltpu.HBM) for a in inputs])

    def send(what, pair, flip):
        return lax.ppermute(what, AXES, swapped(count_x, count_y, pair, flip))

    side = send(edge, None, True)
    low_near = send(near, 1, False)
    side_low = send(side, 1, False)
    low_far = send(far, 1, False)
    high_near = send(near, 0, False)
    high_far = send(far, 0, False)
    side_high = send(side, 0, False)
    piece = shape((count, layers * HALF * cols), bf16)
    spread, square, *dev = pl.pallas_call(
        functools.partial(local_kernel, geom),
        out_shape=(shape((rows * count, cols), f32), shape((count, count), f32)) + (piece,) * 6,
        compiler_params=params,
        name="local",
    )(near, far, table)
    up = pl.pallas_call(
        functools.partial(upper_kernel, geom),
        out_shape=shape((layers * 4 * count, wide), f32),
        compiler_params=params,
        name="upper",
    )(near, far, high_near, high_far, side, side_high, spread)
    parts = [pltpu.VMEM((2 * count, piece.shape[1]), bf16)] * 3
    mid, grad_near, grad_far, hess_far, spread_two, with_dev, total = pl.pallas_call(
        functools.partial(middle_kernel, geom),
        out_shape=(
            shape((half, wide), f32),
            shape((half, cols), f32),
            shape((half, cols), f32),
            shape((half, cols), f32),
            shape((HALF * count, cols), f32),
            shape((2 * count, count), f32),
            shape((2 * count, 2 * count), f32),
        ),
        scratch_shapes=parts,
        compiler_params=params,
        name="middle",
    )(near, far, low_near, side, side_low, spread, up, table, *dev[3:])
    full = pltpu.VMEM((7 * count // 4, LANES), f32)
    hess_near, mine, other = pl.pallas_call(
        functools.partial(lower_kernel, geom),
        out_shape=(shape((half, cols), f32),) + (shape((7 * count // 8, LANES), f32),) * 2,
        scratch_shapes=parts + [pltpu.VMEM((half, wide), f32), full],
        compiler_params=params,
        name="lower",
    )(near, far, low_near, low_far, side, side_low, mid, up, spread_two, square, with_dev, total, *dev[:3])
    mine, other = all_sum(mine, other)
    out = pl.pallas_call(
        functools.partial(mix_kernel, geom, total_size),
        out_shape=shape(flat.shape, f32),
        scratch_shapes=[full],
        compiler_params=params,
        name="mix",
    )(mine, other, near, far, grad_near, grad_far, hess_near, hess_far, background)
    out = out.reshape(count, layers, tiles, rows, LANES).transpose(0, 1, 3, 2, 4)
    return out.reshape(geom)


def solution(mesh):
    count_x = mesh.shape["gx"]
    sizes = (4, 2, 8, 2) if count_x == 128 else (1, 1, count_x // 2, 2)
    finer = Mesh(mesh.devices.reshape(*sizes, mesh.shape["gy"]), AXES)
    in_specs = (
        P(None, None, GX, "gy"),
        P(None, GX, "gy"),
        P(GX, "gy"),
        P(None, GX, "gy"),
        P(GX, "gy"),
        P(GX, "gy"),
    )
    out_specs = P(None, None, GX, "gy")
    return jax.shard_map(per_device, mesh=finer, in_specs=in_specs, out_specs=out_specs, check_vma=False)
```

```python
import functools

import jax
import jax.numpy as jnp
from jax import lax
from jax.experimental import pallas as pl
from jax.experimental.pallas import tpu as pltpu
from jax.sharding import Mesh
from jax.sharding import PartitionSpec as P

TILE = 4
HALF = TILE // 2
LANES = 128
GX = ("gx_0", "gx_1", "gx_2", "gx_3")
AXES = GX + ("gy",)

prior_weight = 0.05
couple_weight = 0.5
epsilon = 1e-06
highest = lax.Precision.HIGHEST
f32 = jnp.float32
bf16 = jnp.bfloat16


def nn(a, b):
    return lax.dot_general(a, b, (((1,), (0,)), ((), ())), precision=highest, preferred_element_type=f32)


def nt(a, b):
    return lax.dot_general(a, b, (((1,), (1,)), ((), ())), precision=highest, preferred_element_type=f32)


def pieces(a):
    hi = a.astype(bf16)
    rest = a - hi.astype(f32)
    mid = rest.astype(bf16)
    return hi, mid, (rest - mid.astype(f32)).astype(bf16)


def dot_exact(a, table, dims):
    return sum(
        lax.dot_general(part, table, (dims, ((), ())), preferred_element_type=f32)
        for part in pieces(a)[::-1]
    )


def own_table(mask_row, tile, cols):
    pattern = jnp.concatenate(mask_row * (8 // TILE), axis=0)
    full = jnp.concatenate([pattern] * (cols // 8), axis=0)
    which = lax.broadcasted_iota(jnp.int32, (cols, LANES), 0).astype(jnp.int32) // TILE
    return jnp.where(which.astype(f32) == tile, full, 0.0).astype(bf16)


def stored_row(ref, l, r, rows, flip):
    return jnp.where(flip == 1, ref[l, rows - 1 - r : rows - r, :], ref[l, r : r + 1, :])


def pack_kernel(
    geom, part_hbm, back_hbm, tile_hbm, mask_hbm, value_hbm, var_hbm, near_ref, far_ref, edge_ref, table_ref,
    part_ref, back_ref, tile_ref, mask_ref, value_ref, var_ref, sems,
):
    count, layers, rows, cols = geom
    tiles = cols // LANES
    per = layers * rows * tiles
    pairs = (
        (mask_hbm, mask_ref), (tile_hbm, tile_ref), (value_hbm, value_ref), (var_hbm, var_ref),
        (back_hbm, back_ref), (part_hbm, part_ref),
    )
    copies = [pltpu.make_async_copy(src, dst, sems.at[k]) for k, (src, dst) in enumerate(pairs)]
    for copy in copies:
        copy.start()
    flip = lax.axis_index("gx_3")
    lane = lax.broadcasted_iota(jnp.int32, (count, LANES), 1)
    for copy in copies[:5]:
        copy.wait()
    tile = tile_ref[...].astype(f32)
    top = layers * HALF * count + count // tiles
    near_ref[top : top + 8, :] = jnp.zeros((8, cols), f32)
    facts = []
    for r in range(rows):
        source = r + flip * (rows - 1 - 2 * r)
        masks = [mask_ref[source * TILE + c].astype(f32) for c in range(TILE)]
        facts += masks
        table_ref[r * cols : (r + 1) * cols, :] = own_table(masks, tile, cols)
    for k, fact in enumerate(facts + [tile, var_ref[...]]):
        near_ref[top + k // tiles : top + k // tiles + 1, (k % tiles) * LANES : (k % tiles + 1) * LANES] = fact
    copies[5].wait()
    edge = jnp.zeros((count, LANES), f32)
    seen = jnp.zeros((count, LANES), f32)
    for l in range(layers):
        for r in range(rows):
            source = r + flip * (rows - 1 - 2 * r)
            base = (l * rows + r) * 2 * TILE + TILE
            back = stored_row(back_ref, l, r, rows, flip)
            half_ref, start = (near_ref, far_ref)[r // HALF], (l * HALF + r % HALF) * count
            state = []
            for ct in range(tiles):
                cell = part_ref[pl.ds((l * tiles + ct) * rows + source, count, stride=per), :]
                state.append(cell)
                dev = cell - back[:, ct * LANES : (ct + 1) * LANES]
                half_ref[start : start + count, ct * LANES : (ct + 1) * LANES] = dev
                if ct == 0:
                    rolled = pltpu.roll(dev, base, axis=1)
                    edge = jnp.where((lane >= base) & (lane < base + TILE), rolled, edge)
                if ct == tiles - 1:
                    rolled = pltpu.roll(dev, base, axis=1)
                    edge = jnp.where((lane >= base - TILE) & (lane < base), rolled, edge)
            if l == 0:
                table = table_ref[r * cols : (r + 1) * cols, :]
                seen = seen + dot_exact(jnp.concatenate(state, axis=1), table, ((1,), (0,)))
    pull = (0.25 * value_ref[...] - 0.0625 * seen) / var_ref[...]
    for r in range(rows):
        base = (layers * rows + r) * 2 * TILE + TILE
        for start, low in ((0, base), (cols - LANES, base - TILE)):
            table = table_ref[r * cols + start : r * cols + start + LANES, :]
            rolled = pltpu.roll(dot_exact(pull, table, ((1,), (1,))), base, axis=1)
            edge = jnp.where((lane >= low) & (lane < low + TILE), rolled, edge)
    edge_ref[...] = edge
    top = layers * HALF * count
    part = count // tiles
    for ct in range(tiles):
        near_ref[top : top + part, ct * LANES : (ct + 1) * LANES] = pull[ct * part : (ct + 1) * part]


def fetch_main(geom, ref):
    count, layers, _, cols = geom
    tiles = cols // LANES
    top = layers * HALF * count + count // tiles

    def fetch(k):
        return ref[top + k // tiles : top + k // tiles + 1, (k % tiles) * LANES : (k % tiles + 1) * LANES]

    return fetch


def pull_main(geom, ref):
    count, layers, _, cols = geom
    top, tiles = layers * HALF * count, cols // LANES
    part = count // tiles
    return jnp.concatenate([ref[top : top + part, ct * LANES : (ct + 1) * LANES] for ct in range(tiles)], axis=0)


def masks_of(fetch, r):
    return [fetch(r * TILE + c) for c in range(TILE)]


def rows_dot(left, right):
    return lax.dot_general(left, right, (((1,), (1,)), ((), ())), preferred_element_type=f32)


def gram_self(parts):
    hi, mid, lo = (part[...] for part in parts)
    cross = rows_dot(hi, lo)
    total = rows_dot(mid, mid) + (cross + cross.T)
    cross = rows_dot(hi, mid)
    return total + (cross + cross.T) + rows_dot(hi, hi)


def gram_cross(left, right):
    total = 0.0
    for i, j in ((2, 0), (0, 2), (1, 1), (1, 0), (0, 1), (0, 0)):
        total = total + rows_dot(left[i][...], right[j][...])
    return total


def slab_row(halves, count, l, r):
    start = (l * HALF + r % HALF) * count
    return halves[r // HALF][start : start + count, :]


def local_kernel(geom, near_ref, far_ref, table_ref, spread_ref, square_ref, *dev_refs):
    count, layers, rows, cols = geom
    pull = pull_main(geom, near_ref)
    for r in range(rows):
        spread_ref[r * count : (r + 1) * count, :] = dot_exact(
            pull, table_ref[r * cols : (r + 1) * cols, :], ((1,), (1,))
        )
    for l in range(layers):
        for r in range(rows):
            k = l * HALF + r % HALF
            half = dev_refs[3 * (r // HALF) : 3 * (r // HALF) + 3]
            for ref, piece in zip(half, pieces(slab_row((near_ref, far_ref), count, l, r))):
                ref[:, k * cols : (k + 1) * cols] = piece
    square_ref[...] = gram_self(dev_refs[:3]) + gram_self(dev_refs[3:])


def edge_tile(side_ref, slot):
    return pltpu.roll(side_ref[...], LANES - (slot * 2 * TILE + TILE), axis=1)


def smooth(mid, up, down):
    wide = mid.shape[1]
    return 8.0 * mid - (pltpu.roll(mid, 1, axis=1) + pltpu.roll(mid, wide - 1, axis=1) + up + down)


def prior_rows(layers, which, field, store):
    for l in range(layers):
        level = {}
        for r in which:
            for near in (r - 1, r, r + 1):
                if near not in level:
                    level[near] = smooth(field(l, near), field(l, near - 1), field(l, near + 1))
            mine = field(l, r)
            curved = smooth(level[r], level[r - 1], level[r + 1])
            store(l, r, mine, (-prior_weight / 16.0) * (curved + 16.0 * couple_weight * (mine - field(1 - l, r))))


def slab_spread(geom, near_ref, r):
    fetch = fetch_main(geom, near_ref)
    table = own_table(masks_of(fetch, r), fetch(geom[2] * TILE), geom[3])
    return dot_exact(pull_main(geom, near_ref), table, ((1,), (1,)))


def gradient_rows(geom, which, own, other, side_ref, side_other_ref, other_row, spread, out_ref):
    count, layers, rows, _ = geom

    def row_of(r):
        return (own, side_ref, r) if 0 <= r < rows else (other, side_other_ref, other_row(r))

    def field(l, r):
        halves, side, rr = row_of(r)
        return jnp.concatenate([slab_row(halves, count, l, rr), edge_tile(side, l * rows + rr)], axis=1)

    def put(l, r, mine, out):
        if l == 0:
            _, side, rr = row_of(r)
            out = out + jnp.concatenate([spread(r), edge_tile(side, layers * rows + rr)], axis=1)
        start = (l * len(which) + r - which[0]) * count
        out_ref[start : start + count, :] = out

    prior_rows(layers, which, field, put)


def upper_kernel(
    geom, near_ref, far_ref, high_near_ref, high_far_ref, side_ref, side_high_ref, spread_ref, up_ref
):
    count, _, rows, _ = geom
    which = tuple(range(rows - 2, rows + 2))
    own, other = (near_ref, far_ref), (high_near_ref, high_far_ref)
    other_row = lambda r: 2 * rows - 1 - r

    def spread(r):
        if r < rows:
            return spread_ref[r * count : (r + 1) * count, :]
        return slab_spread(geom, high_near_ref, other_row(r))

    gradient_rows(geom, which, own, other, side_ref, side_high_ref, other_row, spread, up_ref)


def gradient_at(count, l, r, down_ref, mid_ref, up_ref):
    if r < 0:
        ref, start = down_ref, (l * 2 + r + 2) * count
    elif r < 2:
        ref, start = mid_ref, (l * 2 + r) * count
    else:
        ref, start = up_ref, (l * 4 + r - 2) * count
    return ref[start : start + count, :]


def linear_rows(geom, which, field, extra, hess_ref, parts):
    count, layers, _, cols = geom

    def put(l, r, mine, out):
        out = out[:, 0:cols]
        if l == 0:
            out = out + extra(r)
        k = l * HALF + r % HALF
        hess_ref[k * count : (k + 1) * count, :] = out
        span = slice(k * cols, (k + 1) * cols)
        for ref, grad, hess in zip(parts, pieces(mine[:, 0:cols]), pieces(out)):
            ref[0:count, span] = grad
            ref[count:, span] = hess

    prior_rows(layers, which, field, put)


def middle_kernel(
    geom, near_ref, far_ref, low_near_ref, side_ref, side_low_ref, spread_ref, up_ref, table_ref,
    dev_hi, dev_mid, dev_lo, mid_ref, grad_near_ref, grad_far_ref, hess_ref, spread_two_ref, spread_low_ref, with_dev_ref,
    self_ref, *parts,
):
    count, layers, rows, cols = geom
    own = (near_ref, far_ref)
    other_row = lambda r: -1 - r
    spread = lambda r: spread_ref[r * count : (r + 1) * count, :]
    gradient_rows(geom, (0, 1), own, (low_near_ref, None), side_ref, side_low_ref, other_row, spread, mid_ref)
    field = lambda l, r: gradient_at(count, l, r, None, mid_ref, up_ref)
    for l in range(layers):
        for r in range(rows):
            start = (l * HALF + r % HALF) * count
            (grad_near_ref, grad_far_ref)[r // HALF][start : start + count, :] = field(l, r)[:, 0:cols]
    table = lambda r: table_ref[r * cols : (r + 1) * cols, :]
    seen = sum(dot_exact(field(0, r)[:, 0:cols], table(r), ((1,), (0,))) for r in range(rows))
    pull = -0.0625 * seen / fetch_main(geom, near_ref)(rows * TILE + 1)
    for r in range(HALF):
        spread_two_ref[r * count : (r + 1) * count, :] = dot_exact(pull, table(r), ((1,), (1,)))
    for r in (-2, -1):
        spread_low_ref[(r + 2) * count : (r + 3) * count, :] = slab_spread(geom, low_near_ref, other_row(r))
    extra = lambda r: dot_exact(pull, table(r), ((1,), (1,)))
    linear_rows(geom, (2, 3), field, extra, hess_ref, parts)
    with_dev_ref[...] = gram_cross(parts, (dev_hi, dev_mid, dev_lo))
    self_ref[...] = gram_self(parts)


def lower_kernel(
    geom, near_ref, far_ref, low_near_ref, low_far_ref, side_ref, side_low_ref, mid_ref, up_ref, spread_two_ref,
    spread_low_ref, square_ref, with_dev_ref, self_ref, dev_hi, dev_mid, dev_lo, hess_ref, mine_ref, other_ref,
    hi_ref, mid_part_ref, lo_ref, down, full,
):
    count, _, _, _ = geom
    own, other = (near_ref, far_ref), (low_near_ref, low_far_ref)
    other_row = lambda r: -1 - r
    spread = lambda r: spread_low_ref[(r + 2) * count : (r + 3) * count, :]
    gradient_rows(geom, (-2, -1), own, other, side_ref, side_low_ref, other_row, spread, down)
    field = lambda l, r: gradient_at(count, l, r, down, mid_ref, up_ref)
    extra = lambda r: spread_two_ref[r * count : (r + 1) * count, :]
    parts = (hi_ref, mid_part_ref, lo_ref)
    linear_rows(geom, (0, 1), field, extra, hess_ref, parts)
    with_dev = gram_cross(parts, (dev_hi, dev_mid, dev_lo)) + with_dev_ref[...]
    total = gram_self(parts) + self_ref[...]
    c = count
    row = lax.broadcasted_iota(jnp.int32, (c, c), 0)
    col = lax.broadcasted_iota(jnp.int32, (c, c), 1)
    eye = jnp.where(row == col, 1.0, 0.0)
    dd = square_ref[...]
    gd, hd = with_dev[0:c], with_dev[c:]
    gg, hg, hh = total[0:c, 0:c], total[c:, 0:c], total[c:, c:]
    h = c // 2
    full[0:c, 0:c] = jnp.where(col >= row, dd, gg)
    full[0:c, c:] = jnp.where(col >= row, hh, hg)
    full[c : c + h, 0:c] = gd[0:h]
    columns = (
        jnp.sum(gg * eye, axis=1, keepdims=True),
        jnp.sum(hg * eye, axis=1, keepdims=True),
        hd[:, 0:1],
        gd[:, 0:1],
    )
    tail = gd[h:]
    for k, column in enumerate(columns):
        for part in range(2):
            tail = jnp.where(col[0:h] == 2 * k + part, column[part * h : (part + 1) * h], tail)
    full[c : c + h, c:] = tail
    flip = lax.axis_index("gx_3")
    half = full.shape[0] // 2
    mine_ref[...] = full[pl.ds(pl.multiple_of(flip * half, 8), half), :]
    other_ref[...] = full[pl.ds(pl.multiple_of((1 - flip) * half, 8), half), :]


def mix_kernel(
    geom, total_size, mine_ref, other_ref, grad_near_ref, grad_far_ref, hess_near_ref, hess_far_ref, part_hbm,
    back_hbm, out_ref, full, part_ref, back_ref, sems,
):
    count, layers, rows, cols = geom
    tiles = cols // LANES
    per = layers * rows * tiles
    copies = [
        pltpu.make_async_copy(part_hbm, part_ref, sems.at[0]),
        pltpu.make_async_copy(back_hbm, back_ref, sems.at[1]),
    ]
    for copy in copies:
        copy.start()
    flip = lax.axis_index("gx_3")
    c = count
    half = mine_ref.shape[0]
    full[pl.ds(pl.multiple_of(flip * half, 8), half), :] = mine_ref[...]
    full[pl.ds(pl.multiple_of((1 - flip) * half, 8), half), :] = other_ref[...]
    row = lax.broadcasted_iota(jnp.int32, (c, c), 0)
    col = lax.broadcasted_iota(jnp.int32, (c, c), 1)
    eye = jnp.where(row == col, 1.0, 0.0)
    pair_count = float(c * (c - 1))
    left, right = full[0:c, 0:c], full[0:c, c:]
    left_t, right_t = left.T, right.T
    h = c // 2
    head, tail = full[c : c + h, 0:c], full[c : c + h, c:]

    def column(k):
        return jnp.concatenate([tail[:, 2 * k : 2 * k + 1], tail[:, 2 * k + 1 : 2 * k + 2]], axis=0)

    dd = jnp.where(col >= row, left, left_t)
    hh = jnp.where(col >= row, right, right_t)
    gg = jnp.where(row > col, left, jnp.where(row < col, left_t, column(0)))
    hg = jnp.where(row > col, right, jnp.where(row < col, right_t, column(1)))
    head_t = jnp.concatenate([head, jnp.zeros((h, c), f32)], axis=0).T
    mirrored = head_t[h:] - (head_t[h:, 0:1] - column(3)[h:]) + (head[0:1] - head_t[0:1])
    gd = jnp.concatenate([head, jnp.where(col[0:h] < h, mirrored, tail)], axis=0)
    hd = gg - (gg[:, 0:1] - column(2))

    def weights(gram):
        distance = (
            jnp.sum(gram * eye, axis=1, keepdims=True) + jnp.sum(gram * eye, axis=0, keepdims=True) - 2.0 * gram
        )
        width = jnp.sum(distance * (1.0 - eye), keepdims=True) / (pair_count * total_size) + epsilon
        kernel = jnp.exp(-distance / (2.0 * width * total_size))
        spread = (eye * jnp.sum(kernel, axis=1, keepdims=True) - kernel) / (width * c)
        return kernel / c, spread

    def step_scale(square_sum):
        return 1.0 / jnp.sqrt(square_sum / (c * total_size) + epsilon)

    push, pull = weights(dd)
    drift_dev = nn(pull, dd) + nn(push, gd)
    drift_grad = nt(pull, gd) + nn(push, gg)
    drift_drift = nt(drift_dev, pull) + nt(drift_grad, push)
    scale = step_scale(jnp.sum(drift_drift * eye, keepdims=True))
    gram = dd + scale * (drift_dev + drift_dev.T) + scale * scale * drift_drift
    push_two, pull_two = weights(gram)
    keep = eye + scale * pull
    gain = scale * push
    on_dev = nn(pull_two, keep)
    on_grad = nn(push_two, keep) + nn(pull_two, gain)
    on_hess = nn(push_two, gain)
    square = jnp.sum(
        nn(on_dev, dd) * on_dev
        + nn(on_grad, gg) * on_grad
        + nn(on_hess, hh) * on_hess
        + 2.0 * (nn(on_grad, gd) * on_dev + nn(on_hess, hd) * on_dev + nn(on_hess, hg) * on_grad),
        keepdims=True,
    )
    scale_two = step_scale(square)
    mix = jnp.concatenate(
        [scale * pull + scale_two * on_dev, gain + scale_two * on_grad, scale_two * on_hess], axis=1
    )
    mix = pieces(mix)
    lefts = (jnp.concatenate(mix, axis=0), jnp.concatenate(mix[:2], axis=0), mix[0])
    for copy in copies:
        copy.wait()
    for l in range(layers):
        for r in range(rows):
            source = r + flip * (rows - 1 - 2 * r)
            places = [pl.ds((l * tiles + ct) * rows + source, c, stride=per) for ct in range(tiles)]
            state = jnp.concatenate([part_ref[place, :] for place in places], axis=1)
            own = state - stored_row(back_ref, l, r, rows, flip)
            grad = slab_row((grad_near_ref, grad_far_ref), c, l, r)
            hess = slab_row((hess_near_ref, hess_far_ref), c, l, r)
            stack = pieces(jnp.concatenate([own, grad, hess], axis=0))
            parts = [
                lax.dot_general(a, b, (((1,), (0,)), ((), ())), preferred_element_type=f32)
                for a, b in zip(lefts, stack)
            ]
            small = parts[0][2 * c :] + parts[1][c:] + parts[2]
            drift = (small + (parts[0][c : 2 * c] + parts[1][0:c])) + parts[0][0:c]
            new = state + drift
            for ct, place in enumerate(places):
                out_ref[place, :] = new[:, ct * LANES : (ct + 1) * LANES]


def all_sum(mine, other):
    swap = [(0, 1), (1, 0)]
    held = mine + lax.ppermute(other, "gx_3", swap)
    for axes in (("gx_2",), ("gx_0", "gx_1", "gy")):
        size = 1
        for axis in axes:
            size *= lax.axis_size(axis)
        copies = jnp.broadcast_to(held, (size,) + held.shape)
        held = jnp.sum(lax.all_to_all(copies, axes, 0, 0, tiled=True), axis=0)
    return held, lax.ppermute(held, "gx_3", swap)


def swapped(count_x, count_y, pair, flip):
    pairs = []
    for x in range(count_x):
        step = 0 if pair is None else (1 if x % 2 == pair else -1)
        target = (x + step) % count_x
        for y in range(count_y):
            pairs.append((x * count_y + y, target * count_y + ((y + 1) % count_y if flip else y)))
    return pairs


def per_device(particles, background, obs_tile, obs_mask, obs_value, obs_var):
    geom = particles.shape
    count, layers, rows, cols = geom
    tiles = cols // LANES
    count_x, count_y = lax.axis_size(GX), lax.axis_size("gy")
    total_size = float(layers * rows * cols * count_x * count_y)
    flat = particles.reshape(count, layers, rows, tiles, LANES).transpose(0, 1, 3, 2, 4)
    flat = flat.reshape(count * layers * rows * tiles, LANES)
    half = layers * HALF * count
    wide = cols + LANES
    params = pltpu.CompilerParams(vmem_limit_bytes=24 * 1024 * 1024)
    shape = jax.ShapeDtypeStruct
    inputs = (flat, background, obs_tile, obs_mask, obs_value, obs_var)
    fixed = [pltpu.with_memory_space_constraint(a, pltpu.HBM) for a in inputs]
    near, far, edge, table = pl.pallas_call(
        functools.partial(pack_kernel, geom),
        out_shape=(
            shape((half + count // tiles + 8, cols), f32),
            shape((half, cols), f32),
            shape((count, LANES), f32),
            shape((rows * cols, LANES), bf16),
        ),
        in_specs=[pl.BlockSpec(memory_space=pltpu.HBM)] * len(inputs),
        scratch_shapes=[pltpu.VMEM(a.shape, a.dtype) for a in inputs] + [pltpu.SemaphoreType.DMA((len(inputs),))],
        compiler_params=params,
        name="pack",
    )(*fixed)

    def send(what, pair, flip):
        return lax.ppermute(what, AXES, swapped(count_x, count_y, pair, flip))

    side = send(edge, None, True)
    low_near = send(near, 1, False)
    side_low = send(side, 1, False)
    low_far = send(far, 1, False)
    high_near = send(near, 0, False)
    high_far = send(far, 0, False)
    side_high = send(side, 0, False)
    piece = shape((count, layers * HALF * cols), bf16)
    spread, square, *dev = pl.pallas_call(
        functools.partial(local_kernel, geom),
        out_shape=(shape((rows * count, cols), f32), shape((count, count), f32)) + (piece,) * 6,
        compiler_params=params,
        name="local",
    )(near, far, table)
    up = pl.pallas_call(
        functools.partial(upper_kernel, geom),
        out_shape=shape((layers * 4 * count, wide), f32),
        compiler_params=params,
        name="upper",
    )(near, far, high_near, high_far, side, side_high, spread)
    parts = [pltpu.VMEM((2 * count, piece.shape[1]), bf16)] * 3
    mid, grad_near, grad_far, hess_far, spread_two, spread_low, with_dev, total = pl.pallas_call(
        functools.partial(middle_kernel, geom),
        out_shape=(
            shape((half, wide), f32),
            shape((half, cols), f32),
            shape((half, cols), f32),
            shape((half, cols), f32),
            shape((HALF * count, cols), f32),
            shape((HALF * count, cols), f32),
            shape((2 * count, count), f32),
            shape((2 * count, 2 * count), f32),
        ),
        scratch_shapes=parts,
        compiler_params=params,
        name="middle",
    )(near, far, low_near, side, side_low, spread, up, table, *dev[3:])
    full = pltpu.VMEM((3 * count // 2, LANES), f32)
    hess_near, mine, other = pl.pallas_call(
        functools.partial(lower_kernel, geom),
        out_shape=(shape((half, cols), f32),) + (shape((3 * count // 4, LANES), f32),) * 2,
        scratch_shapes=parts + [pltpu.VMEM((half, wide), f32), full],
        compiler_params=params,
        name="lower",
    )(near, far, low_near, low_far, side, side_low, mid, up, spread_two, spread_low, square, with_dev, total, *dev[:3])
    mine, other = all_sum(mine, other)
    out = pl.pallas_call(
        functools.partial(mix_kernel, geom, total_size),
        out_shape=shape(flat.shape, f32),
        in_specs=[pl.BlockSpec(memory_space=pltpu.VMEM)] * 6 + [pl.BlockSpec(memory_space=pltpu.HBM)] * 2,
        scratch_shapes=[full, pltpu.VMEM(flat.shape, f32), pltpu.VMEM(background.shape, f32), pltpu.SemaphoreType.DMA((2,))],
        compiler_params=params,
        name="mix",
    )(mine, other, grad_near, grad_far, hess_near, hess_far, *fixed[:2])
    out = out.reshape(count, layers, tiles, rows, LANES).transpose(0, 1, 3, 2, 4)
    return out.reshape(geom)


def solution(mesh):
    count_x = mesh.shape["gx"]
    sizes = (4, 2, 8, 2) if count_x == 128 else (1, 1, count_x // 2, 2)
    finer = Mesh(mesh.devices.reshape(*sizes, mesh.shape["gy"]), AXES)
    in_specs = (
        P(None, None, GX, "gy"),
        P(None, GX, "gy"),
        P(GX, "gy"),
        P(None, GX, "gy"),
        P(GX, "gy"),
        P(GX, "gy"),
    )
    out_specs = P(None, None, GX, "gy")
    return jax.shard_map(per_device, mesh=finer, in_specs=in_specs, out_specs=out_specs, check_vma=False)
```

```python
import functools

import jax
import jax.numpy as jnp
from jax import lax
from jax.experimental import pallas as pl
from jax.experimental.pallas import tpu as pltpu
from jax.sharding import Mesh
from jax.sharding import PartitionSpec as P

TILE = 4
HALF = TILE // 2
LANES = 128
GX = ("gx_0", "gx_1", "gx_2", "gx_3")
AXES = GX + ("gy",)

prior_weight = 0.05
couple_weight = 0.5
epsilon = 1e-06
highest = lax.Precision.HIGHEST
f32 = jnp.float32
bf16 = jnp.bfloat16


def nn(a, b):
    return lax.dot_general(a, b, (((1,), (0,)), ((), ())), precision=highest, preferred_element_type=f32)


def nt(a, b):
    return lax.dot_general(a, b, (((1,), (1,)), ((), ())), precision=highest, preferred_element_type=f32)


def pieces(a):
    hi = a.astype(bf16)
    rest = a - hi.astype(f32)
    mid = rest.astype(bf16)
    return hi, mid, (rest - mid.astype(f32)).astype(bf16)


def dot_exact(a, table, dims):
    return sum(
        lax.dot_general(part, table, (dims, ((), ())), preferred_element_type=f32)
        for part in pieces(a)[::-1]
    )


def own_table(mask_row, tile, cols):
    pattern = jnp.concatenate(mask_row * (8 // TILE), axis=0)
    full = jnp.concatenate([pattern] * (cols // 8), axis=0)
    which = lax.broadcasted_iota(jnp.int32, (cols, LANES), 0).astype(jnp.int32) // TILE
    return jnp.where(which.astype(f32) == tile, full, 0.0).astype(bf16)


def stored_row(ref, l, r, rows, flip):
    return jnp.where(flip == 1, ref[l, rows - 1 - r : rows - r, :], ref[l, r : r + 1, :])


def pack_kernel(
    geom, part_hbm, back_hbm, tile_hbm, mask_hbm, value_hbm, var_hbm, near_ref, far_ref, edge_ref, table_ref,
    part_ref, back_ref, tile_ref, mask_ref, value_ref, var_ref, sems,
):
    count, layers, rows, cols = geom
    tiles = cols // LANES
    spans = [pl.ds(l * rows * tiles, rows * tiles) for l in range(layers)]
    pairs = (
        (mask_hbm, mask_ref), (tile_hbm, tile_ref), (value_hbm, value_ref), (var_hbm, var_ref),
        (back_hbm, back_ref),
    ) + tuple((part_hbm.at[:, span, :], part_ref.at[:, span, :]) for span in spans)
    pitch = part_ref.shape[1]
    lines = part_ref.reshape(count * pitch, LANES)
    copies = [pltpu.make_async_copy(src, dst, sems.at[k]) for k, (src, dst) in enumerate(pairs)]
    for copy in copies:
        copy.start()
    flip = lax.axis_index("gx_3")
    lane = lax.broadcasted_iota(jnp.int32, (count, LANES), 1)
    for copy in copies[:5]:
        copy.wait()
    tile = tile_ref[...].astype(f32)
    top = layers * HALF * count + count // tiles
    near_ref[top : top + 8, :] = jnp.zeros((8, cols), f32)
    facts = []
    for r in range(rows):
        source = r + flip * (rows - 1 - 2 * r)
        masks = [mask_ref[source * TILE + c].astype(f32) for c in range(TILE)]
        facts += masks
        table_ref[r * cols : (r + 1) * cols, :] = own_table(masks, tile, cols)
    for k, fact in enumerate(facts + [tile, var_ref[...]]):
        near_ref[top + k // tiles : top + k // tiles + 1, (k % tiles) * LANES : (k % tiles + 1) * LANES] = fact
    edge = jnp.zeros((count, LANES), f32)
    seen = jnp.zeros((count, LANES), f32)
    for l in range(layers):
        copies[5 + l].wait()
        for r in range(rows):
            source = r + flip * (rows - 1 - 2 * r)
            base = (l * rows + r) * 2 * TILE + TILE
            back = stored_row(back_ref, l, r, rows, flip)
            half_ref, start = (near_ref, far_ref)[r // HALF], (l * HALF + r % HALF) * count
            state = []
            for ct in range(tiles):
                cell = lines[pl.ds((l * tiles + ct) * rows + source, count, stride=pitch), :]
                state.append(cell)
                dev = cell - back[:, ct * LANES : (ct + 1) * LANES]
                half_ref[start : start + count, ct * LANES : (ct + 1) * LANES] = dev
                if ct == 0:
                    rolled = pltpu.roll(dev, base, axis=1)
                    edge = jnp.where((lane >= base) & (lane < base + TILE), rolled, edge)
                if ct == tiles - 1:
                    rolled = pltpu.roll(dev, base, axis=1)
                    edge = jnp.where((lane >= base - TILE) & (lane < base), rolled, edge)
            if l == 0:
                table = table_ref[r * cols : (r + 1) * cols, :]
                seen = seen + dot_exact(jnp.concatenate(state, axis=1), table, ((1,), (0,)))
    pull = (0.25 * value_ref[...] - 0.0625 * seen) / var_ref[...]
    for r in range(rows):
        base = (layers * rows + r) * 2 * TILE + TILE
        for start, low in ((0, base), (cols - LANES, base - TILE)):
            table = table_ref[r * cols + start : r * cols + start + LANES, :]
            rolled = pltpu.roll(dot_exact(pull, table, ((1,), (1,))), base, axis=1)
            edge = jnp.where((lane >= low) & (lane < low + TILE), rolled, edge)
    edge_ref[...] = edge
    top = layers * HALF * count
    part = count // tiles
    for ct in range(tiles):
        near_ref[top : top + part, ct * LANES : (ct + 1) * LANES] = pull[ct * part : (ct + 1) * part]


def fetch_main(geom, ref):
    count, layers, _, cols = geom
    tiles = cols // LANES
    top = layers * HALF * count + count // tiles

    def fetch(k):
        return ref[top + k // tiles : top + k // tiles + 1, (k % tiles) * LANES : (k % tiles + 1) * LANES]

    return fetch


def pull_main(geom, ref):
    count, layers, _, cols = geom
    top, tiles = layers * HALF * count, cols // LANES
    part = count // tiles
    return jnp.concatenate([ref[top : top + part, ct * LANES : (ct + 1) * LANES] for ct in range(tiles)], axis=0)


def masks_of(fetch, r):
    return [fetch(r * TILE + c) for c in range(TILE)]


def rows_dot(left, right):
    return lax.dot_general(left, right, (((1,), (1,)), ((), ())), preferred_element_type=f32)


def gram_self(parts):
    hi, mid, lo = (part[...] for part in parts)
    cross = rows_dot(hi, lo)
    total = rows_dot(mid, mid) + (cross + cross.T)
    cross = rows_dot(hi, mid)
    return total + (cross + cross.T) + rows_dot(hi, hi)


def gram_cross(left, right):
    total = 0.0
    for i, j in ((2, 0), (0, 2), (1, 1), (1, 0), (0, 1), (0, 0)):
        total = total + rows_dot(left[i][...], right[j][...])
    return total


def slab_row(halves, count, l, r):
    start = (l * HALF + r % HALF) * count
    return halves[r // HALF][start : start + count, :]


def local_kernel(geom, near_ref, far_ref, table_ref, spread_ref, square_ref, *dev_refs):
    count, layers, rows, cols = geom
    pull = pull_main(geom, near_ref)
    for r in range(rows):
        spread_ref[r * count : (r + 1) * count, :] = dot_exact(
            pull, table_ref[r * cols : (r + 1) * cols, :], ((1,), (1,))
        )
    for l in range(layers):
        for r in range(rows):
            k = l * HALF + r % HALF
            half = dev_refs[3 * (r // HALF) : 3 * (r // HALF) + 3]
            for ref, piece in zip(half, pieces(slab_row((near_ref, far_ref), count, l, r))):
                ref[:, k * cols : (k + 1) * cols] = piece
    square_ref[...] = gram_self(dev_refs[:3]) + gram_self(dev_refs[3:])


def edge_tile(side_ref, slot):
    return pltpu.roll(side_ref[...], LANES - (slot * 2 * TILE + TILE), axis=1)


def smooth(mid, up, down):
    wide = mid.shape[1]
    return 8.0 * mid - (pltpu.roll(mid, 1, axis=1) + pltpu.roll(mid, wide - 1, axis=1) + up + down)


def prior_rows(layers, which, field, store):
    for l in range(layers):
        level = {}
        for r in which:
            for near in (r - 1, r, r + 1):
                if near not in level:
                    level[near] = smooth(field(l, near), field(l, near - 1), field(l, near + 1))
            mine = field(l, r)
            curved = smooth(level[r], level[r - 1], level[r + 1])
            store(l, r, mine, (-prior_weight / 16.0) * (curved + 16.0 * couple_weight * (mine - field(1 - l, r))))


def slab_spread(geom, near_ref, r):
    fetch = fetch_main(geom, near_ref)
    table = own_table(masks_of(fetch, r), fetch(geom[2] * TILE), geom[3])
    return dot_exact(pull_main(geom, near_ref), table, ((1,), (1,)))


def gradient_rows(geom, which, own, other, side_ref, side_other_ref, other_row, spread, out_ref):
    count, layers, rows, _ = geom

    def row_of(r):
        return (own, side_ref, r) if 0 <= r < rows else (other, side_other_ref, other_row(r))

    def field(l, r):
        halves, side, rr = row_of(r)
        return jnp.concatenate([slab_row(halves, count, l, rr), edge_tile(side, l * rows + rr)], axis=1)

    def put(l, r, mine, out):
        if l == 0:
            _, side, rr = row_of(r)
            out = out + jnp.concatenate([spread(r), edge_tile(side, layers * rows + rr)], axis=1)
        start = (l * len(which) + r - which[0]) * count
        out_ref[start : start + count, :] = out

    prior_rows(layers, which, field, put)


def upper_kernel(
    geom, near_ref, far_ref, high_near_ref, high_far_ref, side_ref, side_high_ref, spread_ref, up_ref
):
    count, _, rows, _ = geom
    which = tuple(range(rows - 2, rows + 2))
    own, other = (near_ref, far_ref), (high_near_ref, high_far_ref)
    other_row = lambda r: 2 * rows - 1 - r

    def spread(r):
        if r < rows:
            return spread_ref[r * count : (r + 1) * count, :]
        return slab_spread(geom, high_near_ref, other_row(r))

    gradient_rows(geom, which, own, other, side_ref, side_high_ref, other_row, spread, up_ref)


def gradient_at(count, l, r, down_ref, mid_ref, up_ref):
    if r < 0:
        ref, start = down_ref, (l * 2 + r + 2) * count
    elif r < 2:
        ref, start = mid_ref, (l * 2 + r) * count
    else:
        ref, start = up_ref, (l * 4 + r - 2) * count
    return ref[start : start + count, :]


def linear_rows(geom, which, field, extra, hess_ref, parts):
    count, layers, _, cols = geom

    def put(l, r, mine, out):
        out = out[:, 0:cols]
        if l == 0:
            out = out + extra(r)
        k = l * HALF + r % HALF
        hess_ref[k * count : (k + 1) * count, :] = out
        span = slice(k * cols, (k + 1) * cols)
        for ref, grad, hess in zip(parts, pieces(mine[:, 0:cols]), pieces(out)):
            ref[0:count, span] = grad
            ref[count:, span] = hess

    prior_rows(layers, which, field, put)


def middle_kernel(
    geom, near_ref, far_ref, low_near_ref, side_ref, side_low_ref, spread_ref, up_ref, table_ref,
    dev_hi, dev_mid, dev_lo, mid_ref, grad_near_ref, grad_far_ref, hess_ref, spread_two_ref, spread_low_ref, with_dev_ref,
    self_ref, *parts,
):
    count, layers, rows, cols = geom
    own = (near_ref, far_ref)
    other_row = lambda r: -1 - r
    spread = lambda r: spread_ref[r * count : (r + 1) * count, :]
    gradient_rows(geom, (0, 1), own, (low_near_ref, None), side_ref, side_low_ref, other_row, spread, mid_ref)
    field = lambda l, r: gradient_at(count, l, r, None, mid_ref, up_ref)
    for l in range(layers):
        for r in range(rows):
            start = (l * HALF + r % HALF) * count
            (grad_near_ref, grad_far_ref)[r // HALF][start : start + count, :] = field(l, r)[:, 0:cols]
    table = lambda r: table_ref[r * cols : (r + 1) * cols, :]
    seen = sum(dot_exact(field(0, r)[:, 0:cols], table(r), ((1,), (0,))) for r in range(rows))
    pull = -0.0625 * seen / fetch_main(geom, near_ref)(rows * TILE + 1)
    for r in range(HALF):
        spread_two_ref[r * count : (r + 1) * count, :] = dot_exact(pull, table(r), ((1,), (1,)))
    for r in (-2, -1):
        spread_low_ref[(r + 2) * count : (r + 3) * count, :] = slab_spread(geom, low_near_ref, other_row(r))
    extra = lambda r: dot_exact(pull, table(r), ((1,), (1,)))
    linear_rows(geom, (2, 3), field, extra, hess_ref, parts)
    with_dev_ref[...] = gram_cross(parts, (dev_hi, dev_mid, dev_lo))
    self_ref[...] = gram_self(parts)


def lower_kernel(
    geom, near_ref, far_ref, low_near_ref, low_far_ref, side_ref, side_low_ref, mid_ref, up_ref, spread_two_ref,
    spread_low_ref, square_ref, with_dev_ref, self_ref, dev_hi, dev_mid, dev_lo, hess_ref, mine_ref, other_ref,
    hi_ref, mid_part_ref, lo_ref, down, full,
):
    count, _, _, _ = geom
    own, other = (near_ref, far_ref), (low_near_ref, low_far_ref)
    other_row = lambda r: -1 - r
    spread = lambda r: spread_low_ref[(r + 2) * count : (r + 3) * count, :]
    gradient_rows(geom, (-2, -1), own, other, side_ref, side_low_ref, other_row, spread, down)
    field = lambda l, r: gradient_at(count, l, r, down, mid_ref, up_ref)
    extra = lambda r: spread_two_ref[r * count : (r + 1) * count, :]
    parts = (hi_ref, mid_part_ref, lo_ref)
    linear_rows(geom, (0, 1), field, extra, hess_ref, parts)
    with_dev = gram_cross(parts, (dev_hi, dev_mid, dev_lo)) + with_dev_ref[...]
    total = gram_self(parts) + self_ref[...]
    c = count
    row = lax.broadcasted_iota(jnp.int32, (c, c), 0)
    col = lax.broadcasted_iota(jnp.int32, (c, c), 1)
    eye = jnp.where(row == col, 1.0, 0.0)
    dd = square_ref[...]
    gd, hd = with_dev[0:c], with_dev[c:]
    gg, hg, hh = total[0:c, 0:c], total[c:, 0:c], total[c:, c:]
    h = c // 2
    full[0:c, 0:c] = jnp.where(col >= row, dd, gg)
    full[0:c, c:] = jnp.where(col >= row, hh, hg)
    full[c : c + h, 0:c] = gd[0:h]
    columns = (
        jnp.sum(gg * eye, axis=1, keepdims=True),
        jnp.sum(hg * eye, axis=1, keepdims=True),
        hd[:, 0:1],
        gd[:, 0:1],
    )
    tail = gd[h:]
    for k, column in enumerate(columns):
        for part in range(2):
            tail = jnp.where(col[0:h] == 2 * k + part, column[part * h : (part + 1) * h], tail)
    full[c : c + h, c:] = tail
    flip = lax.axis_index("gx_3")
    half = full.shape[0] // 2
    mine_ref[...] = full[pl.ds(pl.multiple_of(flip * half, 8), half), :]
    other_ref[...] = full[pl.ds(pl.multiple_of((1 - flip) * half, 8), half), :]


def mix_kernel(
    geom, total_size, mine_ref, other_ref, grad_near_ref, grad_far_ref, hess_near_ref, hess_far_ref, part_hbm,
    back_hbm, out_hbm, full, part_ref, back_ref, dev_hi, dev_mid, dev_lo, rest_hi, rest_mid, rest_lo, sems,
):
    count, layers, rows, cols = geom
    tiles = cols // LANES
    per = layers * rows * tiles
    copies = [
        pltpu.make_async_copy(part_hbm, part_ref.at[:, 0:per, :], sems.at[0]),
        pltpu.make_async_copy(back_hbm, back_ref, sems.at[1]),
    ]
    for copy in copies:
        copy.start()
    flip = lax.axis_index("gx_3")
    c = count
    half = mine_ref.shape[0]
    full[pl.ds(pl.multiple_of(flip * half, 8), half), :] = mine_ref[...]
    full[pl.ds(pl.multiple_of((1 - flip) * half, 8), half), :] = other_ref[...]
    devs, rests = (dev_hi, dev_mid, dev_lo), (rest_hi, rest_mid, rest_lo)
    halves = (grad_near_ref, grad_far_ref), (hess_near_ref, hess_far_ref)
    spans = [slice(k * cols, (k + 1) * cols) for k in range(layers * rows)]
    for l in range(layers):
        for r in range(rows):
            for at, half_refs in enumerate(halves):
                for ref, piece in zip(rests, pieces(slab_row(half_refs, c, l, r))):
                    ref[at * c : (at + 1) * c, spans[l * rows + r]] = piece
    row = lax.broadcasted_iota(jnp.int32, (c, c), 0)
    col = lax.broadcasted_iota(jnp.int32, (c, c), 1)
    eye = jnp.where(row == col, 1.0, 0.0)
    pair_count = float(c * (c - 1))
    left, right = full[0:c, 0:c], full[0:c, c:]
    left_t, right_t = left.T, right.T
    h = c // 2
    head, tail = full[c : c + h, 0:c], full[c : c + h, c:]

    def column(k):
        return jnp.concatenate([tail[:, 2 * k : 2 * k + 1], tail[:, 2 * k + 1 : 2 * k + 2]], axis=0)

    dd = jnp.where(col >= row, left, left_t)
    hh = jnp.where(col >= row, right, right_t)
    gg = jnp.where(row > col, left, jnp.where(row < col, left_t, column(0)))
    hg = jnp.where(row > col, right, jnp.where(row < col, right_t, column(1)))
    head_t = jnp.concatenate([head, jnp.zeros((h, c), f32)], axis=0).T
    mirrored = head_t[h:] - (head_t[h:, 0:1] - column(3)[h:]) + (head[0:1] - head_t[0:1])
    gd = jnp.concatenate([head, jnp.where(col[0:h] < h, mirrored, tail)], axis=0)
    hd = gg - (gg[:, 0:1] - column(2))

    def weights(gram):
        distance = (
            jnp.sum(gram * eye, axis=1, keepdims=True) + jnp.sum(gram * eye, axis=0, keepdims=True) - 2.0 * gram
        )
        width = jnp.sum(distance * (1.0 - eye), keepdims=True) / (pair_count * total_size) + epsilon
        kernel = jnp.exp(-distance / (2.0 * width * total_size))
        spread = (eye * jnp.sum(kernel, axis=1, keepdims=True) - kernel) / (width * c)
        return kernel / c, spread

    def step_scale(square_sum):
        return 1.0 / jnp.sqrt(square_sum / (c * total_size) + epsilon)

    push, pull = weights(dd)
    drift_dev = nn(pull, dd) + nn(push, gd)
    drift_grad = nt(pull, gd) + nn(push, gg)
    drift_drift = nt(drift_dev, pull) + nt(drift_grad, push)
    scale = step_scale(jnp.sum(drift_dev * pull + drift_grad * push, keepdims=True))
    for copy in copies:
        copy.wait()
    pitch = part_ref.shape[1]
    lines = part_ref.reshape(c * pitch, LANES)
    for l in range(layers):
        for r in range(rows):
            source = r + flip * (rows - 1 - 2 * r)
            places = [pl.ds((l * tiles + ct) * rows + source, c, stride=pitch) for ct in range(tiles)]
            state = jnp.concatenate([lines[place, :] for place in places], axis=1)
            own = state - stored_row(back_ref, l, r, rows, flip)
            for ref, piece in zip(devs, pieces(own)):
                ref[:, spans[l * rows + r]] = piece
    gram = dd + scale * (drift_dev + drift_dev.T) + scale * scale * drift_drift
    push_two, pull_two = weights(gram)
    keep = eye + scale * pull
    gain = scale * push
    on_dev = nn(pull_two, keep)
    on_grad = nn(push_two, keep) + nn(pull_two, gain)
    on_hess = nn(push_two, gain)
    square = jnp.sum(
        nn(on_dev, dd) * on_dev
        + nn(on_grad, gg) * on_grad
        + nn(on_hess, hh) * on_hess
        + 2.0 * (nn(on_grad, gd) * on_dev + nn(on_hess, hd) * on_dev + nn(on_hess, hg) * on_grad),
        keepdims=True,
    )
    scale_two = step_scale(square)
    mix = jnp.concatenate(
        [scale * pull + scale_two * on_dev, gain + scale_two * on_grad, scale_two * on_hess], axis=1
    )
    mix = pieces(mix)
    lefts = (jnp.concatenate(mix, axis=0), jnp.concatenate(mix[:2], axis=0), mix[0])
    results = []
    for l in range(layers):
        for r in range(rows):
            source = r + flip * (rows - 1 - 2 * r)
            places = [pl.ds((l * tiles + ct) * rows + source, c, stride=pitch) for ct in range(tiles)]
            state = jnp.concatenate([lines[place, :] for place in places], axis=1)
            span = spans[l * rows + r]
            stack = [jnp.concatenate([d[:, span], o[:, span]], axis=0) for d, o in zip(devs, rests)]
            parts = [
                lax.dot_general(a, b, (((1,), (0,)), ((), ())), preferred_element_type=f32)
                for a, b in zip(lefts, stack)
            ]
            small = parts[0][2 * c :] + parts[1][c:] + parts[2]
            drift = (small + (parts[0][c : 2 * c] + parts[1][0:c])) + parts[0][0:c]
            new = state + drift
            for ct, place in enumerate(places):
                lines[place, :] = new[:, ct * LANES : (ct + 1) * LANES]
        span = pl.ds(l * rows * tiles, rows * tiles)
        results.append(pltpu.make_async_copy(part_ref.at[:, span, :], out_hbm.at[:, span, :], sems.at[2 + l]))
        results[-1].start()
    for result in results:
        result.wait()


def all_sum(mine, other):
    swap = [(0, 1), (1, 0)]
    held = mine + lax.ppermute(other, "gx_3", swap)
    for axes in (("gx_2",), ("gx_0", "gx_1", "gy")):
        size = 1
        for axis in axes:
            size *= lax.axis_size(axis)
        copies = jnp.broadcast_to(held, (size,) + held.shape)
        held = jnp.sum(lax.all_to_all(copies, axes, 0, 0, tiled=True), axis=0)
    return held, lax.ppermute(held, "gx_3", swap)


def swapped(count_x, count_y, pair, flip):
    pairs = []
    for x in range(count_x):
        step = 0 if pair is None else (1 if x % 2 == pair else -1)
        target = (x + step) % count_x
        for y in range(count_y):
            pairs.append((x * count_y + y, target * count_y + ((y + 1) % count_y if flip else y)))
    return pairs


def per_device(particles, background, obs_tile, obs_mask, obs_value, obs_var):
    geom = particles.shape
    count, layers, rows, cols = geom
    tiles = cols // LANES
    count_x, count_y = lax.axis_size(GX), lax.axis_size("gy")
    total_size = float(layers * rows * cols * count_x * count_y)
    flat = particles.reshape(count, layers, rows, tiles, LANES).transpose(0, 1, 3, 2, 4)
    flat = flat.reshape(count, layers * rows * tiles, LANES)
    half = layers * HALF * count
    wide = cols + LANES
    params = pltpu.CompilerParams(vmem_limit_bytes=24 * 1024 * 1024)
    shape = jax.ShapeDtypeStruct
    inputs = (flat, background, obs_tile, obs_mask, obs_value, obs_var)
    fixed = [pltpu.with_memory_space_constraint(a, pltpu.HBM) for a in inputs]
    near, far, edge, table = pl.pallas_call(
        functools.partial(pack_kernel, geom),
        out_shape=(
            shape((half + count // tiles + 8, cols), f32),
            shape((half, cols), f32),
            shape((count, LANES), f32),
            shape((rows * cols, LANES), bf16),
        ),
        in_specs=[pl.BlockSpec(memory_space=pltpu.HBM)] * len(inputs),
        scratch_shapes=[pltpu.VMEM((count, flat.shape[1] + 8, LANES), f32)]
        + [pltpu.VMEM(a.shape, a.dtype) for a in inputs[1:]]
        + [pltpu.SemaphoreType.DMA((len(inputs) + layers - 1,))],
        compiler_params=params,
        name="pack",
    )(*fixed)

    def send(what, pair, flip):
        return lax.ppermute(what, AXES, swapped(count_x, count_y, pair, flip))

    side = send(edge, None, True)
    low_near = send(near, 1, False)
    side_low = send(side, 1, False)
    low_far = send(far, 1, False)
    high_near = send(near, 0, False)
    high_far = send(far, 0, False)
    side_high = send(side, 0, False)
    piece = shape((count, layers * HALF * cols), bf16)
    spread, square, *dev = pl.pallas_call(
        functools.partial(local_kernel, geom),
        out_shape=(shape((rows * count, cols), f32), shape((count, count), f32)) + (piece,) * 6,
        compiler_params=params,
        name="local",
    )(near, far, table)
    up = pl.pallas_call(
        functools.partial(upper_kernel, geom),
        out_shape=shape((layers * 4 * count, wide), f32),
        compiler_params=params,
        name="upper",
    )(near, far, high_near, high_far, side, side_high, spread)
    parts = [pltpu.VMEM((2 * count, piece.shape[1]), bf16)] * 3
    mid, grad_near, grad_far, hess_far, spread_two, spread_low, with_dev, total = pl.pallas_call(
        functools.partial(middle_kernel, geom),
        out_shape=(
            shape((half, wide), f32),
            shape((half, cols), f32),
            shape((half, cols), f32),
            shape((half, cols), f32),
            shape((HALF * count, cols), f32),
            shape((HALF * count, cols), f32),
            shape((2 * count, count), f32),
            shape((2 * count, 2 * count), f32),
        ),
        scratch_shapes=parts,
        compiler_params=params,
        name="middle",
    )(near, far, low_near, side, side_low, spread, up, table, *dev[3:])
    full = pltpu.VMEM((3 * count // 2, LANES), f32)
    hess_near, mine, other = pl.pallas_call(
        functools.partial(lower_kernel, geom),
        out_shape=(shape((half, cols), f32),) + (shape((3 * count // 4, LANES), f32),) * 2,
        scratch_shapes=parts + [pltpu.VMEM((half, wide), f32), full],
        compiler_params=params,
        name="lower",
    )(near, far, low_near, low_far, side, side_low, mid, up, spread_two, spread_low, square, with_dev, total, *dev[:3])
    mine, other = all_sum(mine, other)
    out = pl.pallas_call(
        functools.partial(mix_kernel, geom, total_size),
        out_shape=shape(flat.shape, f32),
        in_specs=[pl.BlockSpec(memory_space=pltpu.VMEM)] * 6 + [pl.BlockSpec(memory_space=pltpu.HBM)] * 2,
        out_specs=pl.BlockSpec(memory_space=pltpu.HBM),
        scratch_shapes=[full, pltpu.VMEM((count, flat.shape[1] + 8, LANES), f32), pltpu.VMEM(background.shape, f32)]
        + [pltpu.VMEM((k * count, layers * rows * cols), bf16) for k in (1, 1, 1, 2, 2, 2)]
        + [pltpu.SemaphoreType.DMA((2 + layers,))],
        compiler_params=params,
        name="mix",
    )(mine, other, grad_near, grad_far, hess_near, hess_far, *fixed[:2])
    out = out.reshape(count, layers, tiles, rows, LANES).transpose(0, 1, 3, 2, 4)
    return out.reshape(geom)


def solution(mesh):
    count_x = mesh.shape["gx"]
    sizes = (4, 2, 8, 2) if count_x == 128 else (1, 1, count_x // 2, 2)
    finer = Mesh(mesh.devices.reshape(*sizes, mesh.shape["gy"]), AXES)
    in_specs = (
        P(None, None, GX, "gy"),
        P(None, GX, "gy"),
        P(GX, "gy"),
        P(None, GX, "gy"),
        P(GX, "gy"),
        P(GX, "gy"),
    )
    out_specs = P(None, None, GX, "gy")
    return jax.shard_map(per_device, mesh=finer, in_specs=in_specs, out_specs=out_specs, check_vma=False)
```

```python
import functools

import jax
import jax.numpy as jnp
from jax import lax
from jax.experimental import pallas as pl
from jax.experimental.pallas import tpu as pltpu
from jax.sharding import Mesh
from jax.sharding import PartitionSpec as P

TILE = 4
HALF = TILE // 2
LANES = 128
GX = ("gx_0", "gx_1", "gx_2", "gx_3")
AXES = GX + ("gy",)

prior_weight = 0.05
couple_weight = 0.5
epsilon = 1e-06
highest = lax.Precision.HIGHEST
f32 = jnp.float32
bf16 = jnp.bfloat16


def nn(a, b):
    return lax.dot_general(a, b, (((1,), (0,)), ((), ())), precision=highest, preferred_element_type=f32)


def nt(a, b):
    return lax.dot_general(a, b, (((1,), (1,)), ((), ())), precision=highest, preferred_element_type=f32)


def pieces(a):
    hi = a.astype(bf16)
    rest = a - hi.astype(f32)
    mid = rest.astype(bf16)
    return hi, mid, (rest - mid.astype(f32)).astype(bf16)


def dot_exact(a, table, dims):
    return sum(
        lax.dot_general(part, table, (dims, ((), ())), preferred_element_type=f32)
        for part in pieces(a)[::-1]
    )


def own_table(mask_row, tile, cols):
    pattern = jnp.concatenate(mask_row * (8 // TILE), axis=0)
    full = jnp.concatenate([pattern] * (cols // 8), axis=0)
    which = lax.broadcasted_iota(jnp.int32, (cols, LANES), 0).astype(jnp.int32) // TILE
    return jnp.where(which.astype(f32) == tile, full, 0.0).astype(bf16)


def stored_row(ref, l, r, rows, flip):
    return jnp.where(flip == 1, ref[l, rows - 1 - r : rows - r, :], ref[l, r : r + 1, :])


def pack_kernel(
    geom, part_hbm, back_hbm, tile_hbm, mask_hbm, value_hbm, var_hbm, near_ref, far_ref, edge_ref, table_ref,
    part_ref, back_ref, tile_ref, mask_ref, value_ref, var_ref, sems,
):
    count, layers, rows, cols = geom
    tiles = cols // LANES
    spans = [pl.ds(l * rows * tiles, rows * tiles) for l in range(layers)]
    pairs = (
        (mask_hbm, mask_ref), (tile_hbm, tile_ref), (value_hbm, value_ref), (var_hbm, var_ref),
        (back_hbm, back_ref),
    ) + tuple((part_hbm.at[:, span, :], part_ref.at[:, span, :]) for span in spans)
    pitch = part_ref.shape[1]
    lines = part_ref.reshape(count * pitch, LANES)
    copies = [pltpu.make_async_copy(src, dst, sems.at[k]) for k, (src, dst) in enumerate(pairs)]
    for copy in copies:
        copy.start()
    flip = lax.axis_index("gx_3")
    lane = lax.broadcasted_iota(jnp.int32, (count, LANES), 1)
    for copy in copies[:5]:
        copy.wait()
    tile = tile_ref[...].astype(f32)
    top = layers * HALF * count + count // tiles
    near_ref[top : top + 8, :] = jnp.zeros((8, cols), f32)
    facts = []
    for r in range(rows):
        source = r + flip * (rows - 1 - 2 * r)
        masks = [mask_ref[source * TILE + c].astype(f32) for c in range(TILE)]
        facts += masks
        table_ref[r * cols : (r + 1) * cols, :] = own_table(masks, tile, cols)
    for k, fact in enumerate(facts + [tile, var_ref[...]]):
        near_ref[top + k // tiles : top + k // tiles + 1, (k % tiles) * LANES : (k % tiles + 1) * LANES] = fact
    edge = jnp.zeros((count, LANES), f32)
    seen = jnp.zeros((count, LANES), f32)
    for l in range(layers):
        copies[5 + l].wait()
        for r in range(rows):
            source = r + flip * (rows - 1 - 2 * r)
            base = (l * rows + r) * 2 * TILE + TILE
            back = stored_row(back_ref, l, r, rows, flip)
            half_ref, start = (near_ref, far_ref)[r // HALF], (l * HALF + r % HALF) * count
            state = []
            for ct in range(tiles):
                cell = lines[pl.ds((l * tiles + ct) * rows + source, count, stride=pitch), :]
                state.append(cell)
                dev = cell - back[:, ct * LANES : (ct + 1) * LANES]
                half_ref[start : start + count, ct * LANES : (ct + 1) * LANES] = dev
                if ct == 0:
                    rolled = pltpu.roll(dev, base, axis=1)
                    edge = jnp.where((lane >= base) & (lane < base + TILE), rolled, edge)
                if ct == tiles - 1:
                    rolled = pltpu.roll(dev, base, axis=1)
                    edge = jnp.where((lane >= base - TILE) & (lane < base), rolled, edge)
            if l == 0:
                table = table_ref[r * cols : (r + 1) * cols, :]
                seen = seen + dot_exact(jnp.concatenate(state, axis=1), table, ((1,), (0,)))
    pull = (0.25 * value_ref[...] - 0.0625 * seen) / var_ref[...]
    for r in range(rows):
        base = (layers * rows + r) * 2 * TILE + TILE
        for start, low in ((0, base), (cols - LANES, base - TILE)):
            table = table_ref[r * cols + start : r * cols + start + LANES, :]
            rolled = pltpu.roll(dot_exact(pull, table, ((1,), (1,))), base, axis=1)
            edge = jnp.where((lane >= low) & (lane < low + TILE), rolled, edge)
    edge_ref[...] = edge
    top = layers * HALF * count
    part = count // tiles
    for ct in range(tiles):
        near_ref[top : top + part, ct * LANES : (ct + 1) * LANES] = pull[ct * part : (ct + 1) * part]


def fetch_main(geom, ref):
    count, layers, _, cols = geom
    tiles = cols // LANES
    top = layers * HALF * count + count // tiles

    def fetch(k):
        return ref[top + k // tiles : top + k // tiles + 1, (k % tiles) * LANES : (k % tiles + 1) * LANES]

    return fetch


def pull_main(geom, ref):
    count, layers, _, cols = geom
    top, tiles = layers * HALF * count, cols // LANES
    part = count // tiles
    return jnp.concatenate([ref[top : top + part, ct * LANES : (ct + 1) * LANES] for ct in range(tiles)], axis=0)


def masks_of(fetch, r):
    return [fetch(r * TILE + c) for c in range(TILE)]


def rows_dot(left, right):
    return lax.dot_general(left, right, (((1,), (1,)), ((), ())), preferred_element_type=f32)


def gram_self(parts):
    hi, mid, lo = (part[...] for part in parts)
    cross = rows_dot(hi, lo)
    total = rows_dot(mid, mid) + (cross + cross.T)
    cross = rows_dot(hi, mid)
    return total + (cross + cross.T) + rows_dot(hi, hi)


def gram_cross(left, right):
    total = 0.0
    for i, j in ((2, 0), (0, 2), (1, 1), (1, 0), (0, 1), (0, 0)):
        total = total + rows_dot(left[i][...], right[j][...])
    return total


def slab_row(halves, count, l, r):
    start = (l * HALF + r % HALF) * count
    return halves[r // HALF][start : start + count, :]


def local_kernel(geom, near_ref, far_ref, table_ref, spread_ref, square_ref, *dev_refs):
    count, layers, rows, cols = geom
    pull = pull_main(geom, near_ref)
    for r in range(rows):
        spread_ref[r * count : (r + 1) * count, :] = dot_exact(
            pull, table_ref[r * cols : (r + 1) * cols, :], ((1,), (1,))
        )
    for l in range(layers):
        for r in range(rows):
            k = l * HALF + r % HALF
            half = dev_refs[3 * (r // HALF) : 3 * (r // HALF) + 3]
            for ref, piece in zip(half, pieces(slab_row((near_ref, far_ref), count, l, r))):
                ref[:, k * cols : (k + 1) * cols] = piece
    square_ref[...] = gram_self(dev_refs[:3]) + gram_self(dev_refs[3:])


def edge_tile(side_ref, slot):
    return pltpu.roll(side_ref[...], LANES - (slot * 2 * TILE + TILE), axis=1)


def smooth(mid, up, down):
    wide = mid.shape[1]
    return 8.0 * mid - (pltpu.roll(mid, 1, axis=1) + pltpu.roll(mid, wide - 1, axis=1) + up + down)


def prior_rows(layers, which, field, store):
    for l in range(layers):
        level = {}
        for r in which:
            for near in (r - 1, r, r + 1):
                if near not in level:
                    level[near] = smooth(field(l, near), field(l, near - 1), field(l, near + 1))
            mine = field(l, r)
            curved = smooth(level[r], level[r - 1], level[r + 1])
            store(l, r, mine, (-prior_weight / 16.0) * (curved + 16.0 * couple_weight * (mine - field(1 - l, r))))


def slab_spread(geom, near_ref, r):
    fetch = fetch_main(geom, near_ref)
    table = own_table(masks_of(fetch, r), fetch(geom[2] * TILE), geom[3])
    return dot_exact(pull_main(geom, near_ref), table, ((1,), (1,)))


def gradient_rows(geom, which, own, other, side_ref, side_other_ref, other_row, spread, out_ref):
    count, layers, rows, _ = geom

    def row_of(r):
        return (own, side_ref, r) if 0 <= r < rows else (other, side_other_ref, other_row(r))

    def field(l, r):
        halves, side, rr = row_of(r)
        return jnp.concatenate([slab_row(halves, count, l, rr), edge_tile(side, l * rows + rr)], axis=1)

    def put(l, r, mine, out):
        if l == 0:
            _, side, rr = row_of(r)
            out = out + jnp.concatenate([spread(r), edge_tile(side, layers * rows + rr)], axis=1)
        start = (l * len(which) + r - which[0]) * count
        out_ref[start : start + count, :] = out

    prior_rows(layers, which, field, put)


def upper_kernel(
    geom, near_ref, far_ref, high_near_ref, high_far_ref, side_ref, side_high_ref, spread_ref, up_ref
):
    count, _, rows, _ = geom
    which = tuple(range(rows - 2, rows + 2))
    own, other = (near_ref, far_ref), (high_near_ref, high_far_ref)
    other_row = lambda r: 2 * rows - 1 - r

    def spread(r):
        if r < rows:
            return spread_ref[r * count : (r + 1) * count, :]
        return slab_spread(geom, high_near_ref, other_row(r))

    gradient_rows(geom, which, own, other, side_ref, side_high_ref, other_row, spread, up_ref)


def gradient_at(count, l, r, down_ref, mid_ref, up_ref):
    if r < 0:
        ref, start = down_ref, (l * 2 + r + 2) * count
    elif r < 2:
        ref, start = mid_ref, (l * 2 + r) * count
    else:
        ref, start = up_ref, (l * 4 + r - 2) * count
    return ref[start : start + count, :]


def linear_rows(geom, which, field, extra, hess_ref, parts):
    count, layers, _, cols = geom

    def put(l, r, mine, out):
        out = out[:, 0:cols]
        if l == 0:
            out = out + extra(r)
        k = l * HALF + r % HALF
        hess_ref[k * count : (k + 1) * count, :] = out
        span = slice(k * cols, (k + 1) * cols)
        for ref, grad, hess in zip(parts, pieces(mine[:, 0:cols]), pieces(out)):
            ref[0:count, span] = grad
            ref[count:, span] = hess

    prior_rows(layers, which, field, put)


def middle_kernel(
    geom, near_ref, far_ref, low_near_ref, side_ref, side_low_ref, spread_ref, up_ref, table_ref,
    dev_hi, dev_mid, dev_lo, mid_ref, grad_near_ref, grad_far_ref, hess_ref, spread_two_ref, spread_low_ref, with_dev_ref,
    self_ref, *parts,
):
    count, layers, rows, cols = geom
    own = (near_ref, far_ref)
    other_row = lambda r: -1 - r
    spread = lambda r: spread_ref[r * count : (r + 1) * count, :]
    gradient_rows(geom, (0, 1), own, (low_near_ref, None), side_ref, side_low_ref, other_row, spread, mid_ref)
    field = lambda l, r: gradient_at(count, l, r, None, mid_ref, up_ref)
    for l in range(layers):
        for r in range(rows):
            start = (l * HALF + r % HALF) * count
            (grad_near_ref, grad_far_ref)[r // HALF][start : start + count, :] = field(l, r)[:, 0:cols]
    table = lambda r: table_ref[r * cols : (r + 1) * cols, :]
    seen = sum(dot_exact(field(0, r)[:, 0:cols], table(r), ((1,), (0,))) for r in range(rows))
    pull = -0.0625 * seen / fetch_main(geom, near_ref)(rows * TILE + 1)
    for r in range(HALF):
        spread_two_ref[r * count : (r + 1) * count, :] = dot_exact(pull, table(r), ((1,), (1,)))
    for r in (-2, -1):
        spread_low_ref[(r + 2) * count : (r + 3) * count, :] = slab_spread(geom, low_near_ref, other_row(r))
    extra = lambda r: dot_exact(pull, table(r), ((1,), (1,)))
    linear_rows(geom, (2, 3), field, extra, hess_ref, parts)
    with_dev_ref[...] = gram_cross(parts, (dev_hi, dev_mid, dev_lo))
    self_ref[...] = gram_self(parts)


def lower_kernel(
    geom, near_ref, far_ref, low_near_ref, low_far_ref, side_ref, side_low_ref, mid_ref, up_ref, spread_two_ref,
    spread_low_ref, square_ref, with_dev_ref, self_ref, dev_hi, dev_mid, dev_lo, hess_ref, mine_ref, other_ref,
    hi_ref, mid_part_ref, lo_ref, down, full,
):
    count, _, _, _ = geom
    own, other = (near_ref, far_ref), (low_near_ref, low_far_ref)
    other_row = lambda r: -1 - r
    spread = lambda r: spread_low_ref[(r + 2) * count : (r + 3) * count, :]
    gradient_rows(geom, (-2, -1), own, other, side_ref, side_low_ref, other_row, spread, down)
    field = lambda l, r: gradient_at(count, l, r, down, mid_ref, up_ref)
    extra = lambda r: spread_two_ref[r * count : (r + 1) * count, :]
    parts = (hi_ref, mid_part_ref, lo_ref)
    linear_rows(geom, (0, 1), field, extra, hess_ref, parts)
    with_dev = gram_cross(parts, (dev_hi, dev_mid, dev_lo)) + with_dev_ref[...]
    total = gram_self(parts) + self_ref[...]
    c = count
    row = lax.broadcasted_iota(jnp.int32, (c, c), 0)
    col = lax.broadcasted_iota(jnp.int32, (c, c), 1)
    eye = jnp.where(row == col, 1.0, 0.0)
    dd = square_ref[...]
    gd, hd = with_dev[0:c], with_dev[c:]
    gg, hg, hh = total[0:c, 0:c], total[c:, 0:c], total[c:, c:]
    h = c // 2
    full[0:c, 0:c] = jnp.where(col >= row, dd, gg)
    full[0:c, c:] = jnp.where(col >= row, hh, hg)
    full[c : c + h, 0:c] = gd[0:h]
    columns = (
        jnp.sum(gg * eye, axis=1, keepdims=True),
        jnp.sum(hg * eye, axis=1, keepdims=True),
        hd[:, 0:1],
        gd[:, 0:1],
    )
    tail = gd[h:]
    for k, column in enumerate(columns):
        for part in range(2):
            tail = jnp.where(col[0:h] == 2 * k + part, column[part * h : (part + 1) * h], tail)
    full[c : c + h, c:] = tail
    flip = lax.axis_index("gx_3")
    half = full.shape[0] // 2
    mine_ref[...] = full[pl.ds(pl.multiple_of(flip * half, 8), half), :]
    other_ref[...] = full[pl.ds(pl.multiple_of((1 - flip) * half, 8), half), :]


def mix_kernel(
    geom, total_size, mine_ref, other_ref, grad_near_ref, grad_far_ref, hess_near_ref, hess_far_ref, part_hbm,
    back_hbm, out_hbm, full, part_ref, back_ref, sems,
):
    count, layers, rows, cols = geom
    tiles = cols // LANES
    per = layers * rows * tiles
    copies = [
        pltpu.make_async_copy(part_hbm, part_ref.at[:, 0:per, :], sems.at[0]),
        pltpu.make_async_copy(back_hbm, back_ref, sems.at[1]),
    ]
    for copy in copies:
        copy.start()
    flip = lax.axis_index("gx_3")
    c = count
    half = mine_ref.shape[0]
    full[pl.ds(pl.multiple_of(flip * half, 8), half), :] = mine_ref[...]
    full[pl.ds(pl.multiple_of((1 - flip) * half, 8), half), :] = other_ref[...]
    row = lax.broadcasted_iota(jnp.int32, (c, c), 0)
    col = lax.broadcasted_iota(jnp.int32, (c, c), 1)
    eye = jnp.where(row == col, 1.0, 0.0)
    pair_count = float(c * (c - 1))
    left, right = full[0:c, 0:c], full[0:c, c:]
    left_t, right_t = left.T, right.T
    h = c // 2
    head, tail = full[c : c + h, 0:c], full[c : c + h, c:]

    def column(k):
        return jnp.concatenate([tail[:, 2 * k : 2 * k + 1], tail[:, 2 * k + 1 : 2 * k + 2]], axis=0)

    dd = jnp.where(col >= row, left, left_t)
    hh = jnp.where(col >= row, right, right_t)
    gg = jnp.where(row > col, left, jnp.where(row < col, left_t, column(0)))
    hg = jnp.where(row > col, right, jnp.where(row < col, right_t, column(1)))
    head_t = jnp.concatenate([head, jnp.zeros((h, c), f32)], axis=0).T
    mirrored = head_t[h:] - (head_t[h:, 0:1] - column(3)[h:]) + (head[0:1] - head_t[0:1])
    gd = jnp.concatenate([head, jnp.where(col[0:h] < h, mirrored, tail)], axis=0)
    hd = gg - (gg[:, 0:1] - column(2))

    def weights(gram):
        distance = (
            jnp.sum(gram * eye, axis=1, keepdims=True) + jnp.sum(gram * eye, axis=0, keepdims=True) - 2.0 * gram
        )
        width = jnp.sum(distance * (1.0 - eye), keepdims=True) / (pair_count * total_size) + epsilon
        kernel = jnp.exp(-distance / (2.0 * width * total_size))
        spread = (eye * jnp.sum(kernel, axis=1, keepdims=True) - kernel) / (width * c)
        return kernel / c, spread

    def step_scale(square_sum):
        return 1.0 / jnp.sqrt(square_sum / (c * total_size) + epsilon)

    push, pull = weights(dd)
    drift_dev = nn(pull, dd) + nn(push, gd)
    drift_grad = nt(pull, gd) + nn(push, gg)
    drift_drift = nt(drift_dev, pull) + nt(drift_grad, push)
    scale = step_scale(jnp.sum(drift_drift * eye, keepdims=True))
    gram = dd + scale * (drift_dev + drift_dev.T) + scale * scale * drift_drift
    push_two, pull_two = weights(gram)
    keep = eye + scale * pull
    gain = scale * push
    on_dev = nn(pull_two, keep)
    on_grad = nn(push_two, keep) + nn(pull_two, gain)
    on_hess = nn(push_two, gain)
    square = jnp.sum(
        nn(on_dev, dd) * on_dev
        + nn(on_grad, gg) * on_grad
        + nn(on_hess, hh) * on_hess
        + 2.0 * (nn(on_grad, gd) * on_dev + nn(on_hess, hd) * on_dev + nn(on_hess, hg) * on_grad),
        keepdims=True,
    )
    scale_two = step_scale(square)
    mix = jnp.concatenate(
        [scale * pull + scale_two * on_dev, gain + scale_two * on_grad, scale_two * on_hess], axis=1
    )
    mix = pieces(mix)
    lefts = (jnp.concatenate(mix, axis=0), jnp.concatenate(mix[:2], axis=0), mix[0])
    for copy in copies:
        copy.wait()
    pitch = part_ref.shape[1]
    lines = part_ref.reshape(c * pitch, LANES)
    results = []
    for l in range(layers):
        for r in range(rows):
            source = r + flip * (rows - 1 - 2 * r)
            places = [pl.ds((l * tiles + ct) * rows + source, c, stride=pitch) for ct in range(tiles)]
            state = jnp.concatenate([lines[place, :] for place in places], axis=1)
            own = state - stored_row(back_ref, l, r, rows, flip)
            grad = slab_row((grad_near_ref, grad_far_ref), c, l, r)
            hess = slab_row((hess_near_ref, hess_far_ref), c, l, r)
            stack = pieces(jnp.concatenate([own, grad, hess], axis=0))
            parts = [
                lax.dot_general(a, b, (((1,), (0,)), ((), ())), preferred_element_type=f32)
                for a, b in zip(lefts, stack)
            ]
            small = parts[0][2 * c :] + parts[1][c:] + parts[2]
            drift = (small + (parts[0][c : 2 * c] + parts[1][0:c])) + parts[0][0:c]
            new = state + drift
            for ct, place in enumerate(places):
                lines[place, :] = new[:, ct * LANES : (ct + 1) * LANES]
        span = pl.ds(l * rows * tiles, rows * tiles)
        results.append(pltpu.make_async_copy(part_ref.at[:, span, :], out_hbm.at[:, span, :], sems.at[2 + l]))
        results[-1].start()
    for result in results:
        result.wait()


def all_sum(mine, other):
    swap = [(0, 1), (1, 0)]
    held = mine + lax.ppermute(other, "gx_3", swap)
    for axes in (("gx_2",), ("gx_0", "gx_1", "gy")):
        size = 1
        for axis in axes:
            size *= lax.axis_size(axis)
        copies = jnp.broadcast_to(held, (size,) + held.shape)
        held = jnp.sum(lax.all_to_all(copies, axes, 0, 0, tiled=True), axis=0)
    return held, lax.ppermute(held, "gx_3", swap)


def swapped(count_x, count_y, pair, flip):
    pairs = []
    for x in range(count_x):
        step = 0 if pair is None else (1 if x % 2 == pair else -1)
        target = (x + step) % count_x
        for y in range(count_y):
            pairs.append((x * count_y + y, target * count_y + ((y + 1) % count_y if flip else y)))
    return pairs


def per_device(particles, background, obs_tile, obs_mask, obs_value, obs_var):
    geom = particles.shape
    count, layers, rows, cols = geom
    tiles = cols // LANES
    count_x, count_y = lax.axis_size(GX), lax.axis_size("gy")
    total_size = float(layers * rows * cols * count_x * count_y)
    flat = particles.reshape(count, layers, rows, tiles, LANES).transpose(0, 1, 3, 2, 4)
    flat = flat.reshape(count, layers * rows * tiles, LANES)
    half = layers * HALF * count
    wide = cols + LANES
    params = pltpu.CompilerParams(vmem_limit_bytes=24 * 1024 * 1024)
    shape = jax.ShapeDtypeStruct
    inputs = (flat, background, obs_tile, obs_mask, obs_value, obs_var)
    fixed = [pltpu.with_memory_space_constraint(a, pltpu.HBM) for a in inputs]
    near, far, edge, table = pl.pallas_call(
        functools.partial(pack_kernel, geom),
        out_shape=(
            shape((half + count // tiles + 8, cols), f32),
            shape((half, cols), f32),
            shape((count, LANES), f32),
            shape((rows * cols, LANES), bf16),
        ),
        in_specs=[pl.BlockSpec(memory_space=pltpu.HBM)] * len(inputs),
        scratch_shapes=[pltpu.VMEM((count, flat.shape[1] + 8, LANES), f32)]
        + [pltpu.VMEM(a.shape, a.dtype) for a in inputs[1:]]
        + [pltpu.SemaphoreType.DMA((len(inputs) + layers - 1,))],
        compiler_params=params,
        name="pack",
    )(*fixed)

    def send(what, pair, flip):
        return lax.ppermute(what, AXES, swapped(count_x, count_y, pair, flip))

    side = send(edge, None, True)
    low_near = send(near, 1, False)
    side_low = send(side, 1, False)
    low_far = send(far, 1, False)
    high_near = send(near, 0, False)
    high_far = send(far, 0, False)
    side_high = send(side, 0, False)
    piece = shape((count, layers * HALF * cols), bf16)
    spread, square, *dev = pl.pallas_call(
        functools.partial(local_kernel, geom),
        out_shape=(shape((rows * count, cols), f32), shape((count, count), f32)) + (piece,) * 6,
        compiler_params=params,
        name="local",
    )(near, far, table)
    up = pl.pallas_call(
        functools.partial(upper_kernel, geom),
        out_shape=shape((layers * 4 * count, wide), f32),
        compiler_params=params,
        name="upper",
    )(near, far, high_near, high_far, side, side_high, spread)
    parts = [pltpu.VMEM((2 * count, piece.shape[1]), bf16)] * 3
    mid, grad_near, grad_far, hess_far, spread_two, spread_low, with_dev, total = pl.pallas_call(
        functools.partial(middle_kernel, geom),
        out_shape=(
            shape((half, wide), f32),
            shape((half, cols), f32),
            shape((half, cols), f32),
            shape((half, cols), f32),
            shape((HALF * count, cols), f32),
            shape((HALF * count, cols), f32),
            shape((2 * count, count), f32),
            shape((2 * count, 2 * count), f32),
        ),
        scratch_shapes=parts,
        compiler_params=params,
        name="middle",
    )(near, far, low_near, side, side_low, spread, up, table, *dev[3:])
    full = pltpu.VMEM((3 * count // 2, LANES), f32)
    hess_near, mine, other = pl.pallas_call(
        functools.partial(lower_kernel, geom),
        out_shape=(shape((half, cols), f32),) + (shape((3 * count // 4, LANES), f32),) * 2,
        scratch_shapes=parts + [pltpu.VMEM((half, wide), f32), full],
        compiler_params=params,
        name="lower",
    )(near, far, low_near, low_far, side, side_low, mid, up, spread_two, spread_low, square, with_dev, total, *dev[:3])
    mine, other = all_sum(mine, other)
    out = pl.pallas_call(
        functools.partial(mix_kernel, geom, total_size),
        out_shape=shape(flat.shape, f32),
        in_specs=[pl.BlockSpec(memory_space=pltpu.VMEM)] * 6 + [pl.BlockSpec(memory_space=pltpu.HBM)] * 2,
        out_specs=pl.BlockSpec(memory_space=pltpu.HBM),
        scratch_shapes=[full, pltpu.VMEM((count, flat.shape[1] + 8, LANES), f32), pltpu.VMEM(background.shape, f32)]
        + [pltpu.SemaphoreType.DMA((2 + layers,))],
        compiler_params=params,
        name="mix",
    )(mine, other, grad_near, grad_far, hess_near, hess_far, *fixed[:2])
    out = out.reshape(count, layers, tiles, rows, LANES).transpose(0, 1, 3, 2, 4)
    return out.reshape(geom)


def solution(mesh):
    count_x = mesh.shape["gx"]
    sizes = (4, 2, 8, 2) if count_x == 128 else (1, 1, count_x // 2, 2)
    finer = Mesh(mesh.devices.reshape(*sizes, mesh.shape["gy"]), AXES)
    in_specs = (
        P(None, None, GX, "gy"),
        P(None, GX, "gy"),
        P(GX, "gy"),
        P(None, GX, "gy"),
        P(GX, "gy"),
        P(GX, "gy"),
    )
    out_specs = P(None, None, GX, "gy")
    return jax.shard_map(per_device, mesh=finer, in_specs=in_specs, out_specs=out_specs, check_vma=False)
```
